8 devices in a mesh: dp: 1 (over z), sp: 8 (over y, x, core).
Axes of the slice: x: 2, y: 2, z: 1, core: 2. Of those that a mesh axis runs over, the one named last changes fastest.
Arguments:
- resid: float32 [32, 2048, 768], P('dp', 'sp')
- pre_norm: float32 [2, 768], replicated
- w_in: bfloat16 [2, 768, 3352], replicated
- conv_w: float32 [2, 1792, 4], replicated
- conv_b: float32 [2, 1792], replicated
- dt_bias: float32 [2, 24], replicated
- a_log: float32 [2, 24], replicated
- d_skip: float32 [2, 24], replicated
- gate_norm: float32 [2, 1, 1536], replicated
- w_out: bfloat16 [2, 1536, 768], replicated
Outputs:
- output 1: float32 [32, 2048, 768], P('dp', 'sp')
- output 2: float32 [32, 2, 24, 64, 128], P('dp', None, 'sp')
- output 3: bfloat16 [32, 2, 1792, 3], P('dp')
All inputs are finite; a program needn't handle non-finite values.
Results may differ from the reference program's by a relative error of at most 0.0179264.
Values are sent between devices in bfloat16 or wider.
A program may use at most 1 GiB of HBM per device.

```python
import jax
import jax.numpy as jnp
from jax import lax

D_MODEL = 768
D_INNER = 1536
NUM_HEADS = 24
HEAD_DIM = 64
NUM_GROUPS = 1
D_STATE = 128
BATCH = 32
SEQ_LEN = 2048
LAYERS = 2
CONV_WIDTH = 4
CHUNK = 256

CONV_DIM = D_INNER + 2 * NUM_GROUPS * D_STATE
IN_DIM = D_INNER + CONV_DIM + NUM_HEADS
PER_GROUP = NUM_HEADS // NUM_GROUPS
GROUP_WIDTH = D_INNER // NUM_GROUPS
EPSILON = 1e-5


def setup_inputs(seed: int = 0, part: int = 0) -> dict:
    key = jax.random.key(seed)
    keys = jax.random.split(key, 9)
    part_key = jax.random.fold_in(key, part)
    resid = jax.random.normal(part_key, (BATCH, SEQ_LEN, D_MODEL), jnp.float32)
    pre_norm = jax.random.uniform(keys[0], (LAYERS, D_MODEL), jnp.float32, 0.5, 1.5)
    w_in = (jax.random.normal(keys[1], (LAYERS, D_MODEL, IN_DIM), jnp.float32) * D_MODEL ** -0.5).astype(jnp.bfloat16)
    bc_weight = 1.5 * (SEQ_LEN * D_STATE) ** -0.25
    column_scale = jnp.concatenate([jnp.full((D_INNER,), 0.5, jnp.float32), jnp.full((2 * NUM_GROUPS * D_STATE,), bc_weight, jnp.float32)])
    conv_w = jax.random.normal(keys[2], (LAYERS, CONV_DIM, CONV_WIDTH), jnp.float32) * column_scale[:, None]
    conv_b = jax.random.normal(keys[3], (LAYERS, CONV_DIM), jnp.float32) * 0.5 * column_scale
    dt_bias = jax.random.uniform(keys[4], (LAYERS, NUM_HEADS), jnp.float32, -1.0, 1.0)
    a_log = jnp.log(jax.random.uniform(keys[5], (LAYERS, NUM_HEADS), jnp.float32, 0.5, 2.0) / SEQ_LEN)
    d_skip = jax.random.uniform(keys[6], (LAYERS, NUM_HEADS), jnp.float32, 0.5, 1.5)
    gate_norm = jax.random.uniform(keys[7], (LAYERS, NUM_GROUPS, GROUP_WIDTH), jnp.float32, 0.5, 1.5)
    w_out = (jax.random.normal(keys[8], (LAYERS, D_INNER, D_MODEL), jnp.float32) * D_INNER ** -0.5).astype(jnp.bfloat16)
    return {'resid': resid, 'pre_norm': pre_norm, 'w_in': w_in, 'conv_w': conv_w, 'conv_b': conv_b, 'dt_bias': dt_bias, 'a_log': a_log, 'd_skip': d_skip, 'gate_norm': gate_norm, 'w_out': w_out}


def rms_norm(values, gain_vec):
    mean_sq = jnp.mean(values * values, axis=-1, keepdims=True)
    return values * lax.rsqrt(mean_sq + EPSILON) * gain_vec


def ssd_sequence(x_sequence, dt_sequence, b_sequence, c_sequence, a_neg):
    n_chunks = SEQ_LEN // CHUNK
    x_scaled = (x_sequence * dt_sequence[:, :, None]).reshape(n_chunks, CHUNK, NUM_GROUPS, PER_GROUP, HEAD_DIM)
    log_decay = (dt_sequence * a_neg).reshape(n_chunks, CHUNK, NUM_GROUPS, PER_GROUP)
    b_chunks = b_sequence.reshape(n_chunks, CHUNK, NUM_GROUPS, D_STATE)
    c_chunks = c_sequence.reshape(n_chunks, CHUNK, NUM_GROUPS, D_STATE)
    causal = jnp.arange(CHUNK)[:, None] >= jnp.arange(CHUNK)[None, :]

    def chunk_step(state, chunk_data):
        x_chunk, log_chunk, b_chunk, c_chunk = chunk_data
        cum_log = jnp.cumsum(log_chunk, axis=0)
        cum_heads = jnp.transpose(cum_log, (1, 2, 0))
        log_diff = cum_heads[:, :, :, None] - cum_heads[:, :, None, :]
        decay_mat = jnp.exp(jnp.where(causal, log_diff, -jnp.inf))
        scores = jnp.einsum('tgn,sgn->gts', c_chunk, b_chunk)
        mix_mat = decay_mat * scores[:, None]
        y_intra = jnp.einsum('ghts,sghp->tghp', mix_mat, x_chunk)
        y_inter = jnp.einsum('tgn,ghpn->tghp', c_chunk, state) * jnp.exp(cum_log)[:, :, :, None]
        to_end = jnp.exp(cum_log[-1] - cum_log)
        new_state = state * jnp.exp(cum_log[-1])[:, :, None, None] + jnp.einsum('sghp,sgn->ghpn', x_chunk * to_end[:, :, :, None], b_chunk)
        return new_state, y_intra + y_inter

    state_zero = jnp.zeros((NUM_GROUPS, PER_GROUP, HEAD_DIM, D_STATE), jnp.float32)
    final, y_chunks = lax.scan(chunk_step, state_zero, (x_scaled, log_decay, b_chunks, c_chunks))
    return y_chunks.reshape(SEQ_LEN, NUM_HEADS, HEAD_DIM), final.reshape(NUM_HEADS, HEAD_DIM, D_STATE)


def mamba_layer(resid, pre_w, w_in_l, conv_w_l, conv_b_l, dt_b, a_log_l, d_l, gate_w, w_out_l):
    normed = rms_norm(resid, pre_w).astype(jnp.bfloat16)
    projected = jnp.dot(normed.reshape(-1, D_MODEL), w_in_l, preferred_element_type=jnp.float32).astype(jnp.bfloat16).reshape(BATCH, SEQ_LEN, IN_DIM)
    gate_z = projected[:, :, :D_INNER]
    xbc = projected[:, :, D_INNER:D_INNER + CONV_DIM]
    dt_raw = projected[:, :, D_INNER + CONV_DIM:]
    padded = jnp.pad(xbc, ((0, 0), (CONV_WIDTH - 1, 0), (0, 0))).astype(jnp.float32)
    conv_out = conv_b_l + sum(padded[:, tap_index:tap_index + SEQ_LEN] * conv_w_l[:, tap_index] for tap_index in range(CONV_WIDTH))
    activated = jax.nn.silu(conv_out).astype(jnp.bfloat16)
    x_act = activated[:, :, :D_INNER].reshape(BATCH, SEQ_LEN, NUM_HEADS, HEAD_DIM)
    b_act = activated[:, :, D_INNER:D_INNER + NUM_GROUPS * D_STATE].reshape(BATCH, SEQ_LEN, NUM_GROUPS, D_STATE)
    c_act = activated[:, :, D_INNER + NUM_GROUPS * D_STATE:].reshape(BATCH, SEQ_LEN, NUM_GROUPS, D_STATE)
    delta = jax.nn.softplus(dt_raw.astype(jnp.float32) + dt_b).astype(jnp.bfloat16)
    a_neg = -jnp.exp(a_log_l)

    def one_sequence(seq_parts):
        x_part, dt_part, b_part, c_part = seq_parts
        return ssd_sequence(x_part.astype(jnp.float32), dt_part.astype(jnp.float32), b_part.astype(jnp.float32), c_part.astype(jnp.float32), a_neg)

    y_ssm, final = lax.map(one_sequence, (x_act, delta, b_act, c_act))
    y_full = (y_ssm + d_l[:, None] * x_act.astype(jnp.float32)).astype(jnp.bfloat16)
    gated = y_full.astype(jnp.float32).reshape(BATCH, SEQ_LEN, D_INNER) * jax.nn.silu(gate_z.astype(jnp.float32))
    grouped = gated.reshape(BATCH, SEQ_LEN, NUM_GROUPS, GROUP_WIDTH)
    normed_y = (grouped * lax.rsqrt(jnp.mean(grouped * grouped, axis=-1, keepdims=True) + EPSILON) * gate_w).astype(jnp.bfloat16)
    out_proj = jnp.dot(normed_y.reshape(-1, D_INNER), w_out_l, preferred_element_type=jnp.float32).reshape(BATCH, SEQ_LEN, D_MODEL)
    tail_rows = jnp.swapaxes(xbc[:, SEQ_LEN - (CONV_WIDTH - 1):], 1, 2)
    return resid + out_proj, final, tail_rows


def reference(resid, pre_norm, w_in, conv_w, conv_b, dt_bias, a_log, d_skip, gate_norm, w_out):
    def layer_step(carry, layer_weights):
        pre_w, w_in_l, conv_w_l, conv_b_l, dt_b, a_log_l, d_l, gate_w, w_out_l = layer_weights
        new_resid, final, tail_rows = mamba_layer(carry, pre_w, w_in_l, conv_w_l, conv_b_l, dt_b, a_log_l, d_l, gate_w, w_out_l)
        return new_resid, (final, tail_rows)

    out_resid, (finals, tails) = lax.scan(layer_step, resid, (pre_norm, w_in, conv_w, conv_b, dt_bias, a_log, d_skip, gate_norm, w_out))
    return out_resid, jnp.swapaxes(finals, 0, 1), jnp.swapaxes(tails, 0, 1)
```

```python
import functools

import jax
import jax.numpy as jnp
from jax import lax
from jax.experimental import pallas as pl
from jax.experimental.pallas import tpu as pltpu
from jax.sharding import PartitionSpec as P

EPSILON = 1e-5
HALO = 8
LANES = 128


def silu(v):
    half = 0.5 * v
    return half + half * jnp.tanh(half)


def softplus(v):
    return jnp.maximum(v, 0.0) + jnp.log1p(jnp.exp(-jnp.abs(v)))


def round_bf16(v):
    return v.astype(jnp.bfloat16).astype(jnp.float32)


def dot(a, b):
    return jnp.dot(a, b, preferred_element_type=jnp.float32)


def layer_kernel(dims, x_ref, pre_ref, w_in_ref, w_dt_ref, conv_w_ref, conv_b_ref, dtb_ref, a_ref, d_ref, gate_ref, w_out_ref, expand_ref,
                 out_ref, state_ref, tail_ref,
                 res_ref, u_ref, s_ref, g_ref, y_ref):
    d_model, d_inner, d_state, heads, seg, chunks = dims
    head_dim = d_inner // heads
    chunk = pl.program_id(0)
    layer = pl.program_id(1)
    quad = 256
    half = seg // 2

    @pl.when(chunk == 0)
    def _():
        u_ref[layer, :, 0:HALO, :] = jnp.zeros(u_ref.shape[1:2] + (HALO, LANES), jnp.float32)
        s_ref[layer] = jnp.zeros(s_ref.shape[1:], jnp.float32)

    @pl.when(chunk > 0)
    def _():
        u_ref[layer, :, 0:HALO, :] = u_ref[layer, :, seg:seg + HALO, :]

    @pl.when(layer == 0)
    def _():
        res_ref[...] = x_ref[0]

    resid = res_ref[...]
    mean_sq = jnp.mean(resid * resid, axis=-1, keepdims=True)
    h = (resid * lax.rsqrt(mean_sq + EPSILON) * pre_ref[layer]).astype(jnp.bfloat16)

    def conv(first_tile, count):
        outs = []
        for j in range(first_tile, first_tile + count):
            cols = slice(j * LANES, (j + 1) * LANES)
            acc = conv_b_ref[layer, :, cols] + u_ref[layer, j, HALO - 3:HALO - 3 + seg, :] * conv_w_ref[layer, 0:1, cols]
            for tap in range(1, 4):
                acc = acc + u_ref[layer, j, HALO - 3 + tap:HALO - 3 + tap + seg, :] * conv_w_ref[layer, tap:tap + 1, cols]
            outs.append(silu(acc).astype(jnp.bfloat16))
        return outs

    def project_conv(first_col):
        u = round_bf16(dot(h, w_in_ref[layer, :, d_inner + first_col:d_inner + first_col + quad]))
        first_tile = first_col // LANES
        for k in range(quad // LANES):
            u_ref[layer, first_tile + k, HALO:HALO + seg, :] = u[:, k * LANES:(k + 1) * LANES]
        return conv(first_tile, quad // LANES)

    dt_raw = round_bf16(dot(h, w_dt_ref[layer]))
    delta = softplus(dt_raw + dtb_ref[layer]).astype(jnp.bfloat16)
    b_act, c_act = project_conv(d_inner)

    rows = lax.broadcasted_iota(jnp.int32, (seg, seg), 0)
    columns = lax.broadcasted_iota(jnp.int32, (seg, seg), 1)
    tri = jnp.where(rows >= columns, 1.0, 0.0).astype(jnp.bfloat16)
    cum = dot(tri, delta) * a_ref[layer]
    cum_t = jnp.transpose(cum)

    scores = lax.dot_general(c_act, b_act, (((1,), (1,)), ((), ())), preferred_element_type=jnp.float32)
    scores = jnp.where(rows >= columns, scores, 0.0)
    scores_top = scores[:half, :half]
    scores_low = scores[half:, :half]
    scores_diag = scores[half:, half:]
    b_t = jnp.transpose(b_act.astype(jnp.float32)).astype(jnp.bfloat16)
    left = lax.broadcasted_iota(jnp.int32, (seg, LANES), 1) < head_dim

    sum_sq = jnp.zeros((seg, LANES), jnp.float32)
    for q in range(d_inner // quad):
        cols = slice(q * quad, (q + 1) * quad)
        x_tiles = project_conv(q * quad)
        x_act = jnp.concatenate(x_tiles, axis=1)
        z = round_bf16(dot(h, w_in_ref[layer, :, cols]))
        x_float = x_act.astype(jnp.float32)
        dt_wide = dot(delta, expand_ref[:, cols])
        x_scaled = x_float * dt_wide
        x_dot = x_scaled.astype(jnp.bfloat16)
        pair_cums = []
        y_heads = []
        for k in range(quad // LANES):
            pair = []
            for i in range(LANES // head_dim):
                head = (q * quad + k * LANES) // head_dim + i
                wide = jnp.broadcast_to(cum[:, head:head + 1], (seg, LANES))
                pair.append(wide)
                row = cum_t[head:head + 1, :]
                lane = k * LANES + i * head_dim
                m_top = jnp.exp(jnp.minimum(wide[:half] - row[:, :half], 0.0)) * scores_top
                m_low = jnp.exp(wide[half:] - row[:, :half]) * scores_low
                m_diag = jnp.exp(jnp.minimum(wide[half:] - row[:, half:], 0.0)) * scores_diag
                x_head = x_dot[:, lane:lane + head_dim]
                top = dot(m_top.astype(jnp.bfloat16), x_head[:half])
                low = dot(jnp.concatenate([m_low.astype(jnp.bfloat16), m_diag.astype(jnp.bfloat16)], axis=1), x_head)
                y_heads.append(jnp.concatenate([top, low], axis=0))
            pair_cums.append(jnp.where(left, pair[0], pair[1]))
        cum_wide = jnp.concatenate(pair_cums, axis=1)
        last = cum_wide[seg - 1:seg, :]
        state = s_ref[layer, :, cols]
        y_inter = dot(c_act, state.astype(jnp.bfloat16))
        y = jnp.concatenate(y_heads, axis=1) + y_inter * jnp.exp(cum_wide) + d_ref[layer, :, cols] * x_float
        x_end = (x_scaled * jnp.exp(last - cum_wide)).astype(jnp.bfloat16)
        s_ref[layer, :, cols] = state * jnp.exp(last) + dot(b_t, x_end)
        gated = round_bf16(y) * silu(z)
        g_ref[:, cols] = gated
        square = gated * gated
        for k in range(quad // LANES):
            sum_sq = sum_sq + square[:, k * LANES:(k + 1) * LANES]

    scale = lax.rsqrt(jnp.sum(sum_sq, axis=-1, keepdims=True) * (1.0 / d_inner) + EPSILON)
    normed = (g_ref[...] * scale * gate_ref[layer]).astype(jnp.bfloat16)
    result = resid + dot(normed, w_out_ref[layer])
    res_ref[...] = result

    @pl.when(layer == 1)
    def _():
        out_ref[0] = result

    @pl.when(chunk == chunks - 1)
    def _():
        tail_ref[layer] = u_ref[layer, :, seg:seg + HALO, :]
        per_device = d_inner // chunks
        final = jnp.transpose(s_ref[layer])
        for k in range(chunks):
            state_ref[k, layer] = final[k * per_device:(k + 1) * per_device, :]


def solution(mesh):
    seg_count = mesh.shape['sp']

    def forward(resid, pre_norm, w_in, conv_w, conv_b, dt_bias, a_log, d_skip, gate_norm, w_out):
        batch, seg, d_model = resid.shape
        layers, d_inner, _ = w_out.shape
        heads = dt_bias.shape[1]
        head_dim = d_inner // heads
        conv_dim = conv_b.shape[1]
        d_state = (conv_dim - d_inner) // 2
        tiles = conv_dim // LANES
        local_heads = heads // seg_count
        pieces = batch // seg_count

        pad = LANES - heads
        w_dt = jnp.pad(w_in[:, :, d_inner + conv_dim:], ((0, 0), (0, 0), (0, pad)))
        dtb = jnp.pad(dt_bias, ((0, 0), (0, pad)))[:, None]
        a_neg = jnp.pad(-jnp.exp(a_log), ((0, 0), (0, pad)))[:, None]
        d_wide = jnp.repeat(d_skip, head_dim, axis=1)[:, None]
        conv_w_t = jnp.swapaxes(conv_w, 1, 2)
        expand = (jnp.arange(LANES)[:, None] == jnp.arange(d_inner)[None, :] // head_dim).astype(jnp.bfloat16)
        params = (pre_norm[:, None], w_in, w_dt, conv_w_t, conv_b[:, None], dtb, a_neg, d_wide, gate_norm, w_out, expand)

        def whole(a):
            return pl.BlockSpec(a.shape, lambda c, l: (0,) * a.ndim, pipeline_mode=pl.Buffered(1))

        flops = 2 * seg * seg_count * layers * (d_model * w_in.shape[2] + d_inner * d_model + 4 * d_inner * seg)
        run = pl.pallas_call(
            functools.partial(layer_kernel, (d_model, d_inner, d_state, heads, seg, seg_count)),
            grid=(seg_count, layers),
            out_shape=(jax.ShapeDtypeStruct((seg_count, seg, d_model), jnp.float32),
                       jax.ShapeDtypeStruct((seg_count, layers, d_inner // seg_count, d_state), jnp.float32),
                       jax.ShapeDtypeStruct((layers, tiles, HALO, LANES), jnp.float32)),
            in_specs=[pl.BlockSpec((1, seg, d_model), lambda c, l: (c, 0, 0))] + [whole(a) for a in params],
            out_specs=(pl.BlockSpec((1, seg, d_model), lambda c, l: (c, 0, 0)),
                       pl.BlockSpec((seg_count, layers, d_inner // seg_count, d_state), lambda c, l: (0, 0, 0, 0)),
                       pl.BlockSpec((layers, tiles, HALO, LANES), lambda c, l: (0, 0, 0, 0))),
            scratch_shapes=[pltpu.VMEM((seg, d_model), jnp.float32),
                            pltpu.VMEM((layers, tiles, HALO + seg, LANES), jnp.float32),
                            pltpu.VMEM((layers, d_state, d_inner), jnp.float32),
                            pltpu.VMEM((seg, d_inner), jnp.float32),
                            pltpu.VMEM((8, LANES), jnp.float32)],
            compiler_params=pltpu.CompilerParams(dimension_semantics=('arbitrary', 'arbitrary'), vmem_limit_bytes=56 * 1024 * 1024),
            cost_estimate=pl.CostEstimate(flops=flops, bytes_accessed=4 * seg * seg_count * d_model * 2, transcendentals=0),
        )

        arrived = [lax.all_to_all(resid[i * seg_count:(i + 1) * seg_count], 'sp', 0, 0) for i in range(pieces)]
        outs, states, tails = [], [], []
        for i in range(pieces):
            out, state, tail = run(arrived[i], *params)
            outs.append(lax.all_to_all(out, 'sp', 0, 0))
            states.append(lax.all_to_all(state, 'sp', 0, 0))
            tails.append(jnp.swapaxes(tail[:, :, HALO - 3:], 2, 3).reshape(layers, conv_dim, 3).astype(jnp.bfloat16))
        result = jnp.concatenate(outs, axis=0)
        ssm_state = jnp.concatenate(states, axis=0).reshape(batch, layers, local_heads, head_dim, d_state)
        conv_state = lax.all_gather(jnp.stack(tails), 'sp', axis=1).reshape(batch, layers, conv_dim, 3)
        return result, ssm_state, conv_state

    return jax.shard_map(forward, mesh=mesh, in_specs=(P('dp', 'sp', None), P(), P(), P(), P(), P(), P(), P(), P(), P()), out_specs=(P('dp', 'sp', None), P('dp', None, 'sp', None, None), P('dp', None, None, None)), check_vma=False)
```

```python
import functools

import jax
import jax.numpy as jnp
from jax import lax
from jax.experimental import pallas as pl
from jax.experimental.pallas import tpu as pltpu
from jax.sharding import PartitionSpec as P

EPSILON = 1e-5
HALO = 8
LANES = 128


def silu(v):
    half = 0.5 * v
    return half + half * jnp.tanh(half)


def softplus(v):
    return jnp.maximum(v, 0.0) + jnp.log1p(jnp.exp(-jnp.abs(v)))


def round_bf16(v):
    return v.astype(jnp.bfloat16).astype(jnp.float32)


def dot(a, b):
    return jnp.dot(a, b, preferred_element_type=jnp.float32)


def forward_kernel(dims, x_hbm, w_in_hbm, w_out_hbm, pre_ref, w_dt_ref, conv_w_ref, conv_b_ref, dtb_ref, a_ref, d_ref, gate_ref, expand_ref,
                   out_hbm, state_hbm, tail_ref,
                   seg_ref, w_in_ref, w_out_ref, u_ref, s_ref, g_ref, stage_ref,
                   w_sem, in_send, in_recv, out_send, out_recv, state_send, state_recv):
    d_inner, heads, seg, chunks, pieces = dims
    head_dim = d_inner // heads
    piece = pl.program_id(0)
    chunk = pl.program_id(1)
    layer = pl.program_id(2)
    me = lax.axis_index('sp')
    quad = 256
    half = seg // 2

    def weight_copies(l):
        return (pltpu.make_async_copy(w_in_hbm.at[l], w_in_ref.at[l], w_sem.at[0, l]),
                pltpu.make_async_copy(w_out_hbm.at[l], w_out_ref.at[l], w_sem.at[1, l]))

    def local_in(p):
        return pltpu.make_async_copy(x_hbm.at[p * chunks + me], seg_ref.at[p, me], in_recv.at[p, me])

    def send_in(p, peer):
        return pltpu.make_async_remote_copy(src_ref=x_hbm.at[p * chunks + peer], dst_ref=seg_ref.at[p, me], send_sem=in_send.at[p, peer],
                                            recv_sem=in_recv.at[p, me], device_id={'sp': peer}, device_id_type=pl.DeviceIdType.MESH)

    def arrive_in(p, peer):
        return pltpu.make_async_remote_copy(src_ref=x_hbm.at[p * chunks + me], dst_ref=seg_ref.at[p, peer], send_sem=in_send.at[p, peer],
                                            recv_sem=in_recv.at[p, peer], device_id={'sp': peer}, device_id_type=pl.DeviceIdType.MESH)

    def local_out(p):
        return pltpu.make_async_copy(seg_ref.at[p, me], out_hbm.at[p * chunks + me], out_recv.at[p, me])

    def send_out(p, peer):
        return pltpu.make_async_remote_copy(src_ref=seg_ref.at[p, peer], dst_ref=out_hbm.at[p * chunks + me], send_sem=out_send.at[p, peer],
                                            recv_sem=out_recv.at[p, me], device_id={'sp': peer}, device_id_type=pl.DeviceIdType.MESH)

    def arrive_out(p, peer):
        return pltpu.make_async_remote_copy(src_ref=seg_ref.at[p, me], dst_ref=out_hbm.at[p * chunks + peer], send_sem=out_send.at[p, peer],
                                            recv_sem=out_recv.at[p, peer], device_id={'sp': peer}, device_id_type=pl.DeviceIdType.MESH)

    def local_state(p, l):
        return pltpu.make_async_copy(stage_ref.at[l, me], state_hbm.at[p * chunks + me, l], state_recv.at[p, l, me])

    def send_state(p, l, peer):
        return pltpu.make_async_remote_copy(src_ref=stage_ref.at[l, peer], dst_ref=state_hbm.at[p * chunks + me, l], send_sem=state_send.at[l, peer],
                                            recv_sem=state_recv.at[p, l, me], device_id={'sp': peer}, device_id_type=pl.DeviceIdType.MESH)

    def arrive_state(p, l, peer):
        return pltpu.make_async_remote_copy(src_ref=stage_ref.at[l, me], dst_ref=state_hbm.at[p * chunks + peer, l], send_sem=state_send.at[l, peer],
                                            recv_sem=state_recv.at[p, l, peer], device_id={'sp': peer}, device_id_type=pl.DeviceIdType.MESH)

    @pl.when((piece == 0) & (chunk == 0) & (layer == 0))
    def _():
        barrier = pltpu.get_barrier_semaphore()
        for k in range(1, chunks):
            pl.semaphore_signal(barrier, inc=1, device_id={'sp': lax.rem(me + k, chunks)}, device_id_type=pl.DeviceIdType.MESH)
        pl.semaphore_wait(barrier, chunks - 1)
        for p in range(pieces):
            local_in(p).start()
            for k in range(1, chunks):
                send_in(p, lax.rem(me + k, chunks)).start()
            if p == 0:
                for l in range(2):
                    for copy in weight_copies(l):
                        copy.start()

    @pl.when((piece == 0) & (chunk == 0))
    def _():
        for copy in weight_copies(layer):
            copy.wait()

    @pl.when((layer == 0) & (chunk == me))
    def _():
        local_in(piece).wait()

    @pl.when((layer == 0) & (chunk != me))
    def _():
        arrive_in(piece, chunk).wait_recv()

    @pl.when(chunk == 0)
    def _():
        u_ref[layer, :, 0:HALO, :] = jnp.zeros(u_ref.shape[1:2] + (HALO, LANES), jnp.float32)
        s_ref[layer] = jnp.zeros(s_ref.shape[1:], jnp.float32)

    @pl.when(chunk > 0)
    def _():
        u_ref[layer, :, 0:HALO, :] = u_ref[layer, :, seg:seg + HALO, :]

    resid = seg_ref[piece, chunk]
    mean_sq = jnp.mean(resid * resid, axis=-1, keepdims=True)
    h = (resid * lax.rsqrt(mean_sq + EPSILON) * pre_ref[layer]).astype(jnp.bfloat16)

    def conv(first_tile, count):
        outs = []
        for j in range(first_tile, first_tile + count):
            cols = slice(j * LANES, (j + 1) * LANES)
            acc = conv_b_ref[layer, :, cols] + u_ref[layer, j, HALO - 3:HALO - 3 + seg, :] * conv_w_ref[layer, 0:1, cols]
            for tap in range(1, 4):
                acc = acc + u_ref[layer, j, HALO - 3 + tap:HALO - 3 + tap + seg, :] * conv_w_ref[layer, tap:tap + 1, cols]
            outs.append(silu(acc).astype(jnp.bfloat16))
        return outs

    def project_conv(first_col):
        u = round_bf16(dot(h, w_in_ref[layer, :, d_inner + first_col:d_inner + first_col + quad]))
        first_tile = first_col // LANES
        for k in range(quad // LANES):
            u_ref[layer, first_tile + k, HALO:HALO + seg, :] = u[:, k * LANES:(k + 1) * LANES]
        return conv(first_tile, quad // LANES)

    dt_raw = round_bf16(dot(h, w_dt_ref[layer]))
    delta = softplus(dt_raw + dtb_ref[layer]).astype(jnp.bfloat16)
    b_act, c_act = project_conv(d_inner)

    rows = lax.broadcasted_iota(jnp.int32, (seg, seg), 0)
    columns = lax.broadcasted_iota(jnp.int32, (seg, seg), 1)
    tri = jnp.where(rows >= columns, 1.0, 0.0).astype(jnp.bfloat16)
    cum = dot(tri, delta) * a_ref[layer]
    cum_t = jnp.transpose(cum)

    scores = lax.dot_general(c_act, b_act, (((1,), (1,)), ((), ())), preferred_element_type=jnp.float32)
    scores = jnp.where(rows >= columns, scores, 0.0)
    scores_top = scores[:half, :half]
    scores_low = scores[half:, :half]
    scores_diag = scores[half:, half:]
    b_t = jnp.transpose(b_act.astype(jnp.float32)).astype(jnp.bfloat16)
    left = lax.broadcasted_iota(jnp.int32, (seg, LANES), 1) < head_dim

    sum_sq = jnp.zeros((seg, LANES), jnp.float32)
    for q in range(d_inner // quad):
        cols = slice(q * quad, (q + 1) * quad)
        x_tiles = project_conv(q * quad)
        x_act = jnp.concatenate(x_tiles, axis=1)
        z = round_bf16(dot(h, w_in_ref[layer, :, cols]))
        x_float = x_act.astype(jnp.float32)
        dt_wide = dot(delta, expand_ref[:, cols])
        x_scaled = x_float * dt_wide
        x_dot = x_scaled.astype(jnp.bfloat16)
        pair_cums = []
        y_heads = []
        for k in range(quad // LANES):
            pair = []
            for i in range(LANES // head_dim):
                head = (q * quad + k * LANES) // head_dim + i
                wide = jnp.broadcast_to(cum[:, head:head + 1], (seg, LANES))
                pair.append(wide)
                row = cum_t[head:head + 1, :]
                lane = k * LANES + i * head_dim
                m_top = jnp.exp(jnp.minimum(wide[:half] - row[:, :half], 0.0)) * scores_top
                m_low = jnp.exp(wide[half:] - row[:, :half]) * scores_low
                m_diag = jnp.exp(jnp.minimum(wide[half:] - row[:, half:], 0.0)) * scores_diag
                x_head = x_dot[:, lane:lane + head_dim]
                top = dot(m_top.astype(jnp.bfloat16), x_head[:half])
                low = dot(jnp.concatenate([m_low.astype(jnp.bfloat16), m_diag.astype(jnp.bfloat16)], axis=1), x_head)
                y_heads.append(jnp.concatenate([top, low], axis=0))
            pair_cums.append(jnp.where(left, pair[0], pair[1]))
        cum_wide = jnp.concatenate(pair_cums, axis=1)
        last = cum_wide[seg - 1:seg, :]
        state = s_ref[layer, :, cols]
        y_inter = dot(c_act, state.astype(jnp.bfloat16))
        y = jnp.concatenate(y_heads, axis=1) + y_inter * jnp.exp(cum_wide) + d_ref[layer, :, cols] * x_float
        x_end = (x_scaled * jnp.exp(last - cum_wide)).astype(jnp.bfloat16)
        s_ref[layer, :, cols] = state * jnp.exp(last) + dot(b_t, x_end)
        gated = round_bf16(y) * silu(z)
        g_ref[:, cols] = gated
        square = gated * gated
        for k in range(quad // LANES):
            sum_sq = sum_sq + square[:, k * LANES:(k + 1) * LANES]

    scale = lax.rsqrt(jnp.sum(sum_sq, axis=-1, keepdims=True) * (1.0 / d_inner) + EPSILON)
    normed = (g_ref[...] * scale * gate_ref[layer]).astype(jnp.bfloat16)
    result = resid + dot(normed, w_out_ref[layer])
    seg_ref[piece, chunk] = result

    @pl.when((layer == 1) & (chunk == me))
    def _():
        local_out(piece).start()

    @pl.when((layer == 1) & (chunk != me))
    def _():
        send_out(piece, chunk).start()

    @pl.when((chunk == chunks - 1) & (piece > 0))
    def _():
        local_state(piece - 1, layer).wait()
        for k in range(1, chunks):
            send_state(piece - 1, layer, lax.rem(me + k, chunks)).wait_send()

    @pl.when(chunk == chunks - 1)
    def _():
        tail_ref[0, layer] = u_ref[layer, :, seg:seg + HALO, :]
        per_device = d_inner // chunks
        final = jnp.transpose(s_ref[layer])
        for k in range(chunks):
            stage_ref[layer, k] = final[k * per_device:(k + 1) * per_device, :]
        local_state(piece, layer).start()
        for k in range(1, chunks):
            send_state(piece, layer, lax.rem(me + k, chunks)).start()

    @pl.when((piece == pieces - 1) & (chunk == chunks - 1) & (layer == 1))
    def _():
        for l in range(2):
            local_state(pieces - 1, l).wait()
        for p in range(pieces):
            local_out(p).wait()
            for k in range(1, chunks):
                peer = lax.rem(me + k, chunks)
                send_in(p, peer).wait_send()
                send_out(p, peer).wait_send()
                arrive_out(p, peer).wait_recv()
                for l in range(2):
                    arrive_state(p, l, peer).wait_recv()
                    if p == pieces - 1:
                        send_state(p, l, peer).wait_send()


def solution(mesh):
    seg_count = mesh.shape['sp']

    def forward(resid, pre_norm, w_in, conv_w, conv_b, dt_bias, a_log, d_skip, gate_norm, w_out):
        batch, seg, d_model = resid.shape
        layers, d_inner, _ = w_out.shape
        heads = dt_bias.shape[1]
        head_dim = d_inner // heads
        conv_dim = conv_b.shape[1]
        d_state = (conv_dim - d_inner) // 2
        tiles = conv_dim // LANES
        local_heads = heads // seg_count
        pieces = batch // seg_count

        pad = LANES - heads
        w_dt = jnp.pad(w_in[:, :, d_inner + conv_dim:], ((0, 0), (0, 0), (0, pad)))
        dtb = jnp.pad(dt_bias, ((0, 0), (0, pad)))[:, None]
        a_neg = jnp.pad(-jnp.exp(a_log), ((0, 0), (0, pad)))[:, None]
        d_wide = jnp.repeat(d_skip, head_dim, axis=1)[:, None]
        conv_w_t = jnp.swapaxes(conv_w, 1, 2)
        expand = (jnp.arange(LANES)[:, None] == jnp.arange(d_inner)[None, :] // head_dim).astype(jnp.bfloat16)
        params = (pre_norm[:, None], w_dt, conv_w_t, conv_b[:, None], dtb, a_neg, d_wide, gate_norm, expand)

        def whole(a):
            return pl.BlockSpec(a.shape, lambda p, c, l: (0,) * a.ndim, pipeline_mode=pl.Buffered(1))

        hbm = pl.BlockSpec(memory_space=pl.ANY)
        per_device = d_inner // seg_count
        out, state, tail = pl.pallas_call(
            functools.partial(forward_kernel, (d_inner, heads, seg, seg_count, pieces)),
            grid=(pieces, seg_count, layers),
            out_shape=(jax.ShapeDtypeStruct((batch, seg, d_model), jnp.float32),
                       jax.ShapeDtypeStruct((batch, layers, per_device, d_state), jnp.float32),
                       jax.ShapeDtypeStruct((pieces, layers, tiles, HALO, LANES), jnp.float32)),
            in_specs=[hbm, hbm, hbm] + [whole(a) for a in params],
            out_specs=(hbm, hbm, pl.BlockSpec((1, layers, tiles, HALO, LANES), lambda p, c, l: (p, 0, 0, 0, 0))),
            scratch_shapes=[pltpu.VMEM((pieces, seg_count, seg, d_model), jnp.float32),
                            pltpu.VMEM(w_in.shape, jnp.bfloat16),
                            pltpu.VMEM(w_out.shape, jnp.bfloat16),
                            pltpu.VMEM((layers, tiles, HALO + seg, LANES), jnp.float32),
                            pltpu.VMEM((layers, d_state, d_inner), jnp.float32),
                            pltpu.VMEM((seg, d_inner), jnp.float32),
                            pltpu.VMEM((layers, seg_count, per_device, d_state), jnp.float32),
                            pltpu.SemaphoreType.DMA((2, layers)),
                            pltpu.SemaphoreType.DMA((pieces, seg_count)),
                            pltpu.SemaphoreType.DMA((pieces, seg_count)),
                            pltpu.SemaphoreType.DMA((pieces, seg_count)),
                            pltpu.SemaphoreType.DMA((pieces, seg_count)),
                            pltpu.SemaphoreType.DMA((layers, seg_count)),
                            pltpu.SemaphoreType.DMA((pieces, layers, seg_count))],
            compiler_params=pltpu.CompilerParams(dimension_semantics=('arbitrary',) * 3, vmem_limit_bytes=67043328, collective_id=0, has_side_effects=True),
        )(resid, w_in, w_out, *params)
        tails = jnp.swapaxes(tail[:, :, :, HALO - 3:], 3, 4).reshape(pieces, layers, conv_dim, 3).astype(jnp.bfloat16)
        conv_state = lax.all_gather(tails, 'sp', axis=1).reshape(batch, layers, conv_dim, 3)
        return out, state.reshape(batch, layers, local_heads, head_dim, d_state), conv_state

    return jax.shard_map(forward, mesh=mesh, in_specs=(P('dp', 'sp', None), P(), P(), P(), P(), P(), P(), P(), P(), P()), out_specs=(P('dp', 'sp', None), P('dp', None, 'sp', None, None), P('dp', None, None, None)), check_vma=False)
```

```python
import functools

import jax
import jax.numpy as jnp
from jax import lax
from jax.experimental import pallas as pl
from jax.experimental.pallas import tpu as pltpu
from jax.sharding import PartitionSpec as P

EPSILON = 1e-5
HALO = 8
LANES = 128
LOG2_E = 1.4426950408889634


def softplus(v):
    return jnp.maximum(v, 0.0) + jnp.log1p(jnp.exp(-jnp.abs(v)))


def round_bf16(v):
    return v.astype(jnp.bfloat16).astype(jnp.float32)


def dot(a, b):
    return jnp.dot(a, b, preferred_element_type=jnp.float32)


def forward_kernel(dims, x_hbm, w_in_hbm, w_out_hbm, pre_ref, conv_w_ref, conv_b_ref, dt_bias_ref, a_log_ref, d_skip_ref, gate_ref,
                   out_hbm, state_hbm, tail_hbm,
                   seg_ref, w_in_ref, w_dt_ref, w_out_ref, raw_ref, row_ref, expand_ref, u_ref, s_ref, g_ref, stage_ref, tail_f_ref, tail_ref,
                   w_sem, raw_sem, in_send, in_recv, out_send, out_recv, state_send, state_recv, tail_send, tail_recv):
    d_inner, heads, seg, chunks, pieces = dims
    head_dim = d_inner // heads
    conv_dim = conv_b_ref.shape[1]
    tiles = conv_dim // LANES
    piece = pl.program_id(0)
    chunk = pl.program_id(1)
    layer = pl.program_id(2)
    me = lax.axis_index('sp')
    quad = 256
    sub = LANES
    blocks = (d_inner + conv_dim) // quad

    def raw_copy(l, j, slot):
        rows = pl.ds(pl.multiple_of(j * quad, quad), quad)
        return pltpu.make_async_copy(w_in_hbm.at[l, rows, :], raw_ref.at[slot], raw_sem.at[slot])

    def raw_dt_copy(l):
        return pltpu.make_async_copy(w_in_hbm.at[l, pl.ds(d_inner + conv_dim, heads), :], raw_ref.at[l, pl.ds(0, heads), :], raw_sem.at[l])

    def w_out_copy(l):
        return pltpu.make_async_copy(w_out_hbm.at[l], w_out_ref.at[l], w_sem.at[l])

    def local_tail(p):
        return pltpu.make_async_copy(tail_ref.at[p], tail_hbm.at[p * chunks + me], tail_recv.at[p, me])

    def send_tail(p, peer):
        return pltpu.make_async_remote_copy(src_ref=tail_ref.at[p], dst_ref=tail_hbm.at[p * chunks + me], send_sem=tail_send.at[p, peer],
                                            recv_sem=tail_recv.at[p, me], device_id={'sp': peer}, device_id_type=pl.DeviceIdType.MESH)

    def arrive_tail(p, peer):
        return pltpu.make_async_remote_copy(src_ref=tail_ref.at[p], dst_ref=tail_hbm.at[p * chunks + peer], send_sem=tail_send.at[p, peer],
                                            recv_sem=tail_recv.at[p, peer], device_id={'sp': peer}, device_id_type=pl.DeviceIdType.MESH)

    def local_in(p):
        return pltpu.make_async_copy(x_hbm.at[p * chunks + me], seg_ref.at[p, me], in_recv.at[p, me])

    def send_in(p, peer):
        return pltpu.make_async_remote_copy(src_ref=x_hbm.at[p * chunks + peer], dst_ref=seg_ref.at[p, me], send_sem=in_send.at[p, peer],
                                            recv_sem=in_recv.at[p, me], device_id={'sp': peer}, device_id_type=pl.DeviceIdType.MESH)

    def arrive_in(p, peer):
        return pltpu.make_async_remote_copy(src_ref=x_hbm.at[p * chunks + me], dst_ref=seg_ref.at[p, peer], send_sem=in_send.at[p, peer],
                                            recv_sem=in_recv.at[p, peer], device_id={'sp': peer}, device_id_type=pl.DeviceIdType.MESH)

    def local_out(p):
        return pltpu.make_async_copy(seg_ref.at[p, me], out_hbm.at[p * chunks + me], out_recv.at[p, me])

    def send_out(p, peer):
        return pltpu.make_async_remote_copy(src_ref=seg_ref.at[p, peer], dst_ref=out_hbm.at[p * chunks + me], send_sem=out_send.at[p, peer],
                                            recv_sem=out_recv.at[p, me], device_id={'sp': peer}, device_id_type=pl.DeviceIdType.MESH)

    def arrive_out(p, peer):
        return pltpu.make_async_remote_copy(src_ref=seg_ref.at[p, me], dst_ref=out_hbm.at[p * chunks + peer], send_sem=out_send.at[p, peer],
                                            recv_sem=out_recv.at[p, peer], device_id={'sp': peer}, device_id_type=pl.DeviceIdType.MESH)

    def local_state(p, l):
        return pltpu.make_async_copy(stage_ref.at[l, me], state_hbm.at[p * chunks + me, l], state_recv.at[p, l, me])

    def send_state(p, l, peer):
        return pltpu.make_async_remote_copy(src_ref=stage_ref.at[l, peer], dst_ref=state_hbm.at[p * chunks + me, l], send_sem=state_send.at[l, peer],
                                            recv_sem=state_recv.at[p, l, me], device_id={'sp': peer}, device_id_type=pl.DeviceIdType.MESH)

    def arrive_state(p, l, peer):
        return pltpu.make_async_remote_copy(src_ref=stage_ref.at[l, me], dst_ref=state_hbm.at[p * chunks + peer, l], send_sem=state_send.at[l, peer],
                                            recv_sem=state_recv.at[p, l, peer], device_id={'sp': peer}, device_id_type=pl.DeviceIdType.MESH)

    left = lax.broadcasted_iota(jnp.int32, (sub, LANES), 1) < head_dim

    @pl.when((piece == 0) & (chunk == 0) & (layer == 0))
    def _():
        for l in range(2):
            w_out_copy(l).start()
            raw_copy(0, l, l).start()
        barrier = pltpu.get_barrier_semaphore()
        for k in range(1, chunks):
            pl.semaphore_signal(barrier, inc=1, device_id={'sp': lax.rem(me + k, chunks)}, device_id_type=pl.DeviceIdType.MESH)
        pl.semaphore_wait(barrier, chunks - 1)
        for p in range(pieces):
            local_in(p).start()
            for k in range(1, chunks):
                send_in(p, lax.rem(me + k, chunks)).start()

        tail_f_ref[...] = jnp.zeros(tail_f_ref.shape, jnp.float32)
        row_ref[...] = jnp.zeros(row_ref.shape, jnp.float32)
        for l in range(2):
            for tap in range(4):
                row_ref[l, tap:tap + 1, 0:conv_dim] = 0.5 * conv_w_ref[l, tap:tap + 1, :]
            row_ref[l, 4:5, 0:conv_dim] = 0.5 * conv_b_ref[l:l + 1, :]
            row_ref[l, 5:6, 0:heads] = dt_bias_ref[l:l + 1, :]
            row_ref[l, 6:7, 0:heads] = -jnp.exp(a_log_ref[l:l + 1, :]) * LOG2_E
            for k in range(d_inner // LANES):
                d_left = jnp.broadcast_to(d_skip_ref[l:l + 1, 2 * k:2 * k + 1], (1, LANES))
                d_right = jnp.broadcast_to(d_skip_ref[l:l + 1, 2 * k + 1:2 * k + 2], (1, LANES))
                row_ref[l, 7:8, k * LANES:(k + 1) * LANES] = jnp.where(left[0:1], d_left, d_right)
        lane_head = lax.shift_right_logical(lax.broadcasted_iota(jnp.int32, expand_ref.shape, 1), 6)
        expand_ref[...] = jnp.where(lax.broadcasted_iota(jnp.int32, expand_ref.shape, 0) == lane_head, 1.0, 0.0).astype(jnp.bfloat16)

        for l in range(2):
            @pl.loop(0, blocks)
            def _(j):
                slot = lax.rem(j, 2)
                raw_copy(l, j, slot).wait()
                w_in_ref[l, :, pl.ds(pl.multiple_of(j * quad, quad), quad)] = jnp.transpose(raw_ref[slot])

                @pl.when(j + 2 < blocks)
                def _():
                    raw_copy(l, j + 2, slot).start()

            if l == 0:
                for j in range(2):
                    raw_copy(1, j, j).start()
        raw_ref[...] = jnp.zeros(raw_ref.shape, jnp.bfloat16)
        for l in range(2):
            raw_dt_copy(l).start()
        for l in range(2):
            raw_dt_copy(l).wait()
            w_dt_ref[l] = jnp.transpose(raw_ref[l, 0:LANES, :])
            w_out_copy(l).wait()

    @pl.when((layer == 0) & (chunk == me))
    def _():
        local_in(piece).wait()

    @pl.when((layer == 0) & (chunk != me))
    def _():
        arrive_in(piece, chunk).wait_recv()

    @pl.when(chunk == 0)
    def _():
        u_ref[layer, :, 0:HALO, :] = jnp.zeros(u_ref.shape[1:2] + (HALO, LANES), jnp.float32)
        s_ref[layer] = jnp.zeros(s_ref.shape[1:], jnp.float32)

    @pl.when(chunk > 0)
    def _():
        u_ref[layer, :, 0:HALO, :] = u_ref[layer, :, seg:seg + HALO, :]

    resid = seg_ref[piece, chunk]
    mean_sq = jnp.mean(resid * resid, axis=-1, keepdims=True)
    h = (resid * lax.rsqrt(mean_sq + EPSILON) * pre_ref[pl.ds(layer, 1), :]).astype(jnp.bfloat16)

    def project(first_col):
        u = round_bf16(dot(h, w_in_ref[layer, :, d_inner + first_col:d_inner + first_col + quad]))
        first_tile = first_col // LANES
        for k in range(quad // LANES):
            u_ref[layer, first_tile + k, HALO:HALO + seg, :] = u[:, k * LANES:(k + 1) * LANES]

    def conv(first_col):
        outs = []
        for j in range(first_col // LANES, (first_col + quad) // LANES):
            cols = slice(j * LANES, (j + 1) * LANES)
            acc = row_ref[layer, 4:5, cols]
            for tap in range(4):
                acc = acc + u_ref[layer, j, HALO - 3 + tap:HALO - 3 + tap + seg, :] * row_ref[layer, tap:tap + 1, cols]
            outs.append((acc + acc * jnp.tanh(acc)).astype(jnp.bfloat16))
        return outs

    dt_raw = round_bf16(dot(h, w_dt_ref[layer]))
    delta = softplus(dt_raw + row_ref[layer, 5:6, 0:LANES]).astype(jnp.bfloat16)
    project(d_inner)
    project(0)
    b_act, c_act = conv(d_inner)

    causal = lax.broadcasted_iota(jnp.int32, (sub, sub), 0) >= lax.broadcasted_iota(jnp.int32, (sub, sub), 1)
    tri = jnp.where(causal, 1.0, 0.0).astype(jnp.bfloat16)
    b_t = jnp.transpose(b_act.astype(jnp.float32)).astype(jnp.bfloat16)
    subs = [slice(i * sub, (i + 1) * sub) for i in range(seg // sub)]
    cums = [dot(tri, delta[rows]) * row_ref[layer, 6:7, 0:LANES] for rows in subs]
    cums_t = [jnp.transpose(cum) for cum in cums]
    scores = [jnp.where(causal, lax.dot_general(c_act[rows], b_act[rows], (((1,), (1,)), ((), ())), preferred_element_type=jnp.float32), 0.0) for rows in subs]

    sum_sq = [jnp.zeros((sub, LANES), jnp.float32) for _ in subs]
    quads = d_inner // quad
    for q in range(quads):
        cols = slice(q * quad, (q + 1) * quad)
        x_tiles = conv(q * quad)
        if q + 1 < quads:
            project((q + 1) * quad)
        z = dot(h, w_in_ref[layer, :, cols]).astype(jnp.bfloat16)
        dt_wide = dot(delta, expand_ref[:, cols])
        state = s_ref[layer, :, cols]
        for i, rows in enumerate(subs):
            y_inter = dot(c_act[rows], state.astype(jnp.bfloat16))
            x_ends = []
            decays = []
            for k in range(quad // LANES):
                lanes = slice(k * LANES, (k + 1) * LANES)
                head = (q * quad + k * LANES) // head_dim
                x_float = x_tiles[k][rows].astype(jnp.float32)
                x_scaled = x_float * dt_wide[rows, lanes]
                x_dot = x_scaled.astype(jnp.bfloat16)
                wide = [jnp.broadcast_to(cums[i][:, head + n:head + n + 1], (sub, LANES)) for n in range(2)]
                mix = [(jnp.exp2(jnp.minimum(wide[n] - cums_t[i][head + n:head + n + 1, :], 0.0)) * scores[i]).astype(jnp.bfloat16) for n in range(2)]
                none = jnp.zeros_like(x_dot)
                pair_rhs = jnp.concatenate([jnp.where(left, x_dot, none), jnp.where(left, none, x_dot)], axis=0)
                y_intra = dot(jnp.concatenate(mix, axis=1), pair_rhs)
                cum_pair = jnp.where(left, wide[0], wide[1])
                last = cum_pair[sub - 1:sub, :]
                x_ends.append((x_scaled * jnp.exp2(last - cum_pair)).astype(jnp.bfloat16))
                decays.append(jnp.exp2(last))
                tile = slice(q * quad + k * LANES, q * quad + (k + 1) * LANES)
                y = y_intra + y_inter[:, lanes] * jnp.exp2(cum_pair) + row_ref[layer, 7:8, tile] * x_float
                z_half = 0.5 * z[rows, lanes].astype(jnp.float32)
                gated = round_bf16(y) * (z_half + z_half * jnp.tanh(z_half))
                g_ref[rows, tile] = gated
                sum_sq[i] = sum_sq[i] + gated * gated
            state = state * jnp.concatenate(decays, axis=1) + dot(b_t[:, rows], jnp.concatenate(x_ends, axis=1))
        s_ref[layer, :, cols] = state

    for i, rows in enumerate(subs):
        scale = lax.rsqrt(jnp.sum(sum_sq[i], axis=-1, keepdims=True) * (1.0 / d_inner) + EPSILON)
        normed = (g_ref[rows, :] * scale * gate_ref[layer]).astype(jnp.bfloat16)
        seg_ref[piece, chunk, rows, :] = resid[rows] + dot(normed, w_out_ref[layer])

    @pl.when((layer == 1) & (chunk == me))
    def _():
        local_out(piece).start()

    @pl.when((layer == 1) & (chunk != me))
    def _():
        send_out(piece, chunk).start()

    @pl.when((chunk == chunks - 1) & (piece > 0))
    def _():
        local_state(piece - 1, layer).wait()
        for k in range(1, chunks):
            send_state(piece - 1, layer, lax.rem(me + k, chunks)).wait_send()

    @pl.when(chunk == chunks - 1)
    def _():
        for j in range(tiles):
            for k in range(3):
                row = k * 2 * 16 + j
                tail_f_ref[pl.ds(layer * 16 + row, 1), :] = u_ref[layer, j, seg + HALO - 3 + k:seg + HALO - 2 + k, :]

        @pl.when(layer == 1)
        def _():
            tail_ref[piece] = tail_f_ref[...].astype(jnp.bfloat16)
            local_tail(piece).start()
            for k in range(1, chunks):
                send_tail(piece, lax.rem(me + k, chunks)).start()

        per_device = d_inner // chunks
        final = jnp.transpose(s_ref[layer])
        for k in range(chunks):
            stage_ref[layer, k] = final[k * per_device:(k + 1) * per_device, :]
        local_state(piece, layer).start()
        for k in range(1, chunks):
            send_state(piece, layer, lax.rem(me + k, chunks)).start()

    @pl.when((piece == pieces - 1) & (chunk == chunks - 1) & (layer == 1))
    def _():
        for l in range(2):
            local_state(pieces - 1, l).wait()
        for p in range(pieces):
            local_out(p).wait()
            local_tail(p).wait()
            for k in range(1, chunks):
                peer = lax.rem(me + k, chunks)
                send_in(p, peer).wait_send()
                send_out(p, peer).wait_send()
                arrive_out(p, peer).wait_recv()
                send_tail(p, peer).wait_send()
                arrive_tail(p, peer).wait_recv()
                for l in range(2):
                    arrive_state(p, l, peer).wait_recv()
                    if p == pieces - 1:
                        send_state(p, l, peer).wait_send()


def solution(mesh):
    seg_count = mesh.shape['sp']

    def forward(resid, pre_norm, w_in, conv_w, conv_b, dt_bias, a_log, d_skip, gate_norm, w_out):
        batch, seg, d_model = resid.shape
        layers, d_inner, _ = w_out.shape
        heads = dt_bias.shape[1]
        head_dim = d_inner // heads
        conv_dim = conv_b.shape[1]
        d_state = (conv_dim - d_inner) // 2
        tiles = conv_dim // LANES
        pieces = batch // seg_count
        per_device = d_inner // seg_count
        params = (pre_norm, jnp.swapaxes(conv_w, 1, 2), conv_b, dt_bias, a_log, d_skip, gate_norm)

        def whole(a):
            return pl.BlockSpec(a.shape, lambda p, c, l: (0,) * a.ndim, pipeline_mode=pl.Buffered(1))

        hbm = pl.BlockSpec(memory_space=pl.ANY)
        out, state, tail = pl.pallas_call(
            functools.partial(forward_kernel, (d_inner, heads, seg, seg_count, pieces)),
            grid=(pieces, seg_count, layers),
            out_shape=(jax.ShapeDtypeStruct((batch, seg, d_model), jnp.float32),
                       jax.ShapeDtypeStruct((batch, layers, per_device, d_state), jnp.float32),
                       jax.ShapeDtypeStruct((batch, 6 * 16, LANES), jnp.bfloat16)),
            in_specs=[hbm, hbm, hbm] + [whole(a) for a in params],
            out_specs=(hbm, hbm, hbm),
            scratch_shapes=[pltpu.VMEM((pieces, seg_count, seg, d_model), jnp.float32),
                            pltpu.VMEM((layers, d_model, d_inner + conv_dim), jnp.bfloat16),
                            pltpu.VMEM((layers, d_model, LANES), jnp.bfloat16),
                            pltpu.VMEM(w_out.shape, jnp.bfloat16),
                            pltpu.VMEM((2, 256, d_model), jnp.bfloat16),
                            pltpu.VMEM((layers, 8, conv_dim), jnp.float32),
                            pltpu.VMEM((LANES, d_inner), jnp.bfloat16),
                            pltpu.VMEM((layers, tiles, HALO + seg, LANES), jnp.float32),
                            pltpu.VMEM((layers, d_state, d_inner), jnp.float32),
                            pltpu.VMEM((seg, d_inner), jnp.float32),
                            pltpu.VMEM((layers, seg_count, per_device, d_state), jnp.float32),
                            pltpu.VMEM((6 * 16, LANES), jnp.float32),
                            pltpu.VMEM((pieces, 6 * 16, LANES), jnp.bfloat16),
                            pltpu.SemaphoreType.DMA((layers,)),
                            pltpu.SemaphoreType.DMA((2,)),
                            pltpu.SemaphoreType.DMA((pieces, seg_count)),
                            pltpu.SemaphoreType.DMA((pieces, seg_count)),
                            pltpu.SemaphoreType.DMA((pieces, seg_count)),
                            pltpu.SemaphoreType.DMA((pieces, seg_count)),
                            pltpu.SemaphoreType.DMA((layers, seg_count)),
                            pltpu.SemaphoreType.DMA((pieces, layers, seg_count)),
                            pltpu.SemaphoreType.DMA((pieces, seg_count)),
                            pltpu.SemaphoreType.DMA((pieces, seg_count))],
            compiler_params=pltpu.CompilerParams(dimension_semantics=('arbitrary',) * 3, vmem_limit_bytes=67043328, collective_id=0, has_side_effects=True),
        )(resid, jnp.swapaxes(w_in, 1, 2), w_out, *params)
        tails = tail.reshape(batch, 3, layers, 16, LANES)[:, :, :, :tiles].reshape(batch, 3, layers, conv_dim)
        return out, state.reshape(batch, layers, heads // seg_count, head_dim, d_state), jnp.transpose(tails, (0, 2, 3, 1))

    return jax.shard_map(forward, mesh=mesh, in_specs=(P('dp', 'sp', None), P(), P(), P(), P(), P(), P(), P(), P(), P()), out_specs=(P('dp', 'sp', None), P('dp', None, 'sp', None, None), P('dp', None, None, None)), check_vma=False)
```

```python
import functools

import jax
import jax.numpy as jnp
from jax import lax
from jax.experimental import pallas as pl
from jax.experimental.pallas import tpu as pltpu
from jax.sharding import PartitionSpec as P

EPSILON = 1e-5
HALO = 8
SLOTS = 4
LANES = 128
LOG2_E = 1.4426950408889634


def softplus(v):
    return jnp.maximum(v, 0.0) + jnp.log1p(jnp.exp(-jnp.abs(v)))


def round_bf16(v):
    return v.astype(jnp.bfloat16).astype(jnp.float32)


def dot(a, b):
    return jnp.dot(a, b, preferred_element_type=jnp.float32)


def forward_kernel(dims, x_ref, w_in_hbm, w_out_hbm, pre_ref, conv_w_ref, conv_b_ref, dt_bias_ref, a_log_ref, d_skip_ref, gate_ref,
                   out_ref, state_hbm, tail_hbm,
                   res_ref, w_in_ref, w_dt_ref, w_out_ref, raw_ref, row_ref, expand_ref, u_ref, s_in_ref, s_out_ref, halo_in_ref, halo_out_ref, halo_f_ref, g_ref,
                   stage_ref, tail_f_ref, tail_ref,
                   w_sem, raw_sem, s_send, s_recv, halo_send, halo_recv, stage_send, stage_recv, tail_send, tail_recv, credit):
    d_inner, heads, seg, devices, batch = dims
    head_dim = d_inner // heads
    conv_dim = conv_b_ref.shape[1]
    tiles = conv_dim // LANES
    prompt = pl.program_id(0)
    layer = pl.program_id(1)
    me = lax.axis_index('sp')
    quad = 256
    sub = LANES
    quads = d_inner // quad
    bc = quads
    groups = ((bc, 0), (1, 2), (3, 4), (5,))
    spot = {b: (n, 6 * i) for n, group in enumerate(groups) for i, b in enumerate(group)}
    blocks = (d_inner + conv_dim) // quad
    steps = batch * 2
    step = prompt * 2 + layer
    slots = s_in_ref.shape[0]
    slot = lax.rem(step, slots)
    last_device = devices - 1
    after = lax.rem(me + 1, devices)
    before = lax.rem(me + devices - 1, devices)
    tail_group = batch // tail_send.shape[0]
    per_device = d_inner // devices

    def raw_copy(l, j, n):
        rows = pl.ds(pl.multiple_of(j * quad, quad), quad)
        return pltpu.make_async_copy(w_in_hbm.at[l, rows, :], raw_ref.at[n], raw_sem.at[n])

    def raw_dt_copy(l):
        return pltpu.make_async_copy(w_in_hbm.at[l, pl.ds(d_inner + conv_dim, heads), :], raw_ref.at[0, pl.ds(0, heads), :], raw_sem.at[0])

    def w_out_copy(l):
        return pltpu.make_async_copy(w_out_hbm.at[l], w_out_ref.at[l], w_sem.at[l])

    def remote(src, dst, send, recv, peer):
        return pltpu.make_async_remote_copy(src_ref=src, dst_ref=dst, send_sem=send, recv_sem=recv, device_id={'sp': peer},
                                            device_id_type=pl.DeviceIdType.MESH)

    def state_copy(n, q, peer):
        cols = pl.ds(q * quad, quad)
        return remote(s_out_ref.at[n, :, cols], s_in_ref.at[n, :, cols], s_send.at[n, q], s_recv.at[n, q], peer)

    def halo_copy(n, group, peer):
        return remote(halo_out_ref.at[n, group], halo_in_ref.at[n, group], halo_send.at[n, group], halo_recv.at[n, group], peer)

    def stage_copy(n, p, l, peer):
        return remote(stage_ref.at[n, peer], state_hbm.at[p, l], stage_send.at[n, peer], stage_recv, peer)

    def stage_local(n, p, l):
        return pltpu.make_async_copy(stage_ref.at[n, me], state_hbm.at[p, l], stage_send.at[n, me])

    def tail_copy(group, peer):
        rows = pl.ds(group * tail_group, tail_group)
        return remote(tail_ref.at[rows], tail_hbm.at[rows], tail_send.at[group, peer], tail_recv, peer)

    def tail_local(group):
        rows = pl.ds(group * tail_group, tail_group)
        return pltpu.make_async_copy(tail_ref.at[rows], tail_hbm.at[rows], tail_send.at[group, me])

    left = lax.broadcasted_iota(jnp.int32, (sub, LANES), 1) < head_dim

    @pl.when(step == 0)
    def _():
        for l in range(2):
            w_out_copy(l).start()
        barrier = pltpu.get_barrier_semaphore()
        for k in range(1, devices):
            pl.semaphore_signal(barrier, inc=1, device_id={'sp': lax.rem(me + k, devices)}, device_id_type=pl.DeviceIdType.MESH)

        tail_f_ref[...] = jnp.zeros(tail_f_ref.shape, jnp.float32)
        halo_f_ref[...] = jnp.zeros(halo_f_ref.shape, jnp.float32)
        row_ref[...] = jnp.zeros(row_ref.shape, jnp.float32)

        @pl.when(me == 0)
        def _():
            s_in_ref[...] = jnp.zeros(s_in_ref.shape, jnp.float32)
            halo_in_ref[...] = jnp.zeros(halo_in_ref.shape, jnp.bfloat16)

        for l in range(2):
            for tap in range(4):
                row_ref[l, tap:tap + 1, 0:conv_dim] = 0.5 * conv_w_ref[l, tap:tap + 1, :]
            row_ref[l, 4:5, 0:conv_dim] = 0.5 * conv_b_ref[l:l + 1, :]
            row_ref[l, 5:6, 0:heads] = dt_bias_ref[l:l + 1, :]
            row_ref[l, 6:7, 0:heads] = -jnp.exp(a_log_ref[l:l + 1, :]) * LOG2_E
            for k in range(d_inner // LANES):
                d_left = jnp.broadcast_to(d_skip_ref[l:l + 1, 2 * k:2 * k + 1], (1, LANES))
                d_right = jnp.broadcast_to(d_skip_ref[l:l + 1, 2 * k + 1:2 * k + 2], (1, LANES))
                row_ref[l, 7:8, k * LANES:(k + 1) * LANES] = jnp.where(left[0:1], d_left, d_right)
        lane_head = lax.shift_right_logical(lax.broadcasted_iota(jnp.int32, expand_ref.shape, 1), 6)
        expand_ref[...] = jnp.where(lax.broadcasted_iota(jnp.int32, expand_ref.shape, 0) == lane_head, 1.0, 0.0).astype(jnp.bfloat16)

        pl.semaphore_wait(barrier, devices - 1)

    @pl.when(prompt == 0)
    def _():
        for j in range(2):
            raw_copy(layer, j, j).start()

        @pl.loop(0, blocks)
        def _(j):
            n = lax.rem(j, 2)
            raw_copy(layer, j, n).wait()
            w_in_ref[layer, :, pl.ds(pl.multiple_of(j * quad, quad), quad)] = jnp.transpose(raw_ref[n])

            @pl.when(j + 2 < blocks)
            def _():
                raw_copy(layer, j + 2, n).start()

        raw_ref[0, 0:LANES, :] = jnp.zeros((LANES, raw_ref.shape[2]), jnp.bfloat16)
        raw_dt_copy(layer).start()
        raw_dt_copy(layer).wait()
        w_dt_ref[layer] = jnp.transpose(raw_ref[0, 0:LANES, :])
        w_out_copy(layer).wait()

    @pl.when((me < last_device) & (step >= slots))
    def _():
        for n in range(len(groups)):
            halo_copy(slot, n, after).wait_send()
        for q in range(quads):
            state_copy(slot, q, after).wait_send()
        pl.semaphore_wait(credit, 1)

    @pl.when(layer == 0)
    def _():
        res_ref[...] = x_ref[0]

    resid = res_ref[...]
    mean_sq = jnp.mean(resid * resid, axis=-1, keepdims=True)
    h = (resid * lax.rsqrt(mean_sq + EPSILON) * pre_ref[pl.ds(layer, 1), :]).astype(jnp.bfloat16)

    def project(b):
        first_col = b * quad
        u = round_bf16(dot(h, w_in_ref[layer, :, d_inner + first_col:d_inner + first_col + quad]))
        for k in range(quad // LANES):
            j = first_col // LANES + k
            lanes = slice(k * LANES, (k + 1) * LANES)
            u_ref[j, HALO:HALO + seg, :] = u[:, lanes]
            group, first = spot[b]
            for tap in range(3):
                row = first + 2 * tap + k
                halo_f_ref[0, group, row:row + 1, :] = u_ref[j, HALO + seg - 3 + tap:HALO + seg - 2 + tap, :]

    def project_group(group):
        for b in groups[group]:
            project(b)
        halo_out_ref[slot, group] = halo_f_ref[0, group].astype(jnp.bfloat16)

    def take_halo(group):
        halo_f_ref[1, group] = halo_in_ref[slot, group].astype(jnp.float32)

    def conv(b):
        outs = []
        for j in range(b * quad // LANES, (b + 1) * quad // LANES):
            cols = slice(j * LANES, (j + 1) * LANES)
            group, first = spot[b]
            for tap in range(3):
                row = first + 2 * tap + j % 2
                u_ref[j, HALO - 3 + tap:HALO - 2 + tap, :] = halo_f_ref[1, group, row:row + 1, :]
            acc = row_ref[layer, 4:5, cols]
            for tap in range(4):
                acc = acc + u_ref[j, HALO - 3 + tap:HALO - 3 + tap + seg, :] * row_ref[layer, tap:tap + 1, cols]
            outs.append((acc + acc * jnp.tanh(acc)).astype(jnp.bfloat16))
        return outs

    dt_raw = round_bf16(dot(h, w_dt_ref[layer]))
    delta = softplus(dt_raw + row_ref[layer, 5:6, 0:LANES]).astype(jnp.bfloat16)
    project_group(0)

    @pl.when(me < last_device)
    def _():
        halo_copy(slot, 0, after).start()

    @pl.when(me > 0)
    def _():
        halo_copy(slot, 0, before).wait_recv()
        state_copy(slot, 0, before).wait_recv()

    take_halo(0)
    b_act, c_act = conv(bc)
    causal = lax.broadcasted_iota(jnp.int32, (sub, sub), 0) >= lax.broadcasted_iota(jnp.int32, (sub, sub), 1)
    tri = jnp.where(causal, 1.0, 0.0).astype(jnp.bfloat16)
    b_t = jnp.transpose(b_act.astype(jnp.float32)).astype(jnp.bfloat16)
    subs = [slice(i * sub, (i + 1) * sub) for i in range(seg // sub)]
    cums = [dot(tri, delta[rows]) * row_ref[layer, 6:7, 0:LANES] for rows in subs]
    cums_t = [jnp.transpose(cum) for cum in cums]
    scores = [jnp.where(causal, lax.dot_general(c_act[rows], b_act[rows], (((1,), (1,)), ((), ())), preferred_element_type=jnp.float32), 0.0) for rows in subs]

    sum_sq = [jnp.zeros((sub, LANES), jnp.float32) for _ in subs]
    for q in range(quads):
        cols = slice(q * quad, (q + 1) * quad)
        x_tiles = conv(q)
        if q + 1 < len(groups):
            project_group(q + 1)
        z = dot(h, w_in_ref[layer, :, cols]).astype(jnp.bfloat16)
        dt_wide = dot(delta, expand_ref[:, cols])
        state = s_in_ref[slot, :, cols]
        for i, rows in enumerate(subs):
            y_inter = dot(c_act[rows], state.astype(jnp.bfloat16))
            x_ends = []
            decays = []
            for k in range(quad // LANES):
                lanes = slice(k * LANES, (k + 1) * LANES)
                head = (q * quad + k * LANES) // head_dim
                x_float = x_tiles[k][rows].astype(jnp.float32)
                x_scaled = x_float * dt_wide[rows, lanes]
                x_dot = x_scaled.astype(jnp.bfloat16)
                wide = [jnp.broadcast_to(cums[i][:, head + n:head + n + 1], (sub, LANES)) for n in range(2)]
                mix = [(jnp.exp2(jnp.minimum(wide[n] - cums_t[i][head + n:head + n + 1, :], 0.0)) * scores[i]).astype(jnp.bfloat16) for n in range(2)]
                none = jnp.zeros_like(x_dot)
                pair_rhs = jnp.concatenate([jnp.where(left, x_dot, none), jnp.where(left, none, x_dot)], axis=0)
                y_intra = dot(jnp.concatenate(mix, axis=1), pair_rhs)
                cum_pair = jnp.where(left, wide[0], wide[1])
                last = cum_pair[sub - 1:sub, :]
                x_ends.append((x_scaled * jnp.exp2(last - cum_pair)).astype(jnp.bfloat16))
                decays.append(jnp.exp2(last))
                tile = slice(q * quad + k * LANES, q * quad + (k + 1) * LANES)
                y = y_intra + y_inter[:, lanes] * jnp.exp2(cum_pair) + row_ref[layer, 7:8, tile] * x_float
                z_half = 0.5 * z[rows, lanes].astype(jnp.float32)
                gated = round_bf16(y) * (z_half + z_half * jnp.tanh(z_half))
                g_ref[rows, tile] = gated
                sum_sq[i] = sum_sq[i] + gated * gated
            state = state * jnp.concatenate(decays, axis=1) + dot(b_t[:, rows], jnp.concatenate(x_ends, axis=1))
        s_out_ref[slot, :, cols] = state

        @pl.when(me < last_device)
        def _():
            state_copy(slot, q, after).start()
            if q + 1 < len(groups):
                halo_copy(slot, q + 1, after).start()

        if q + 1 < quads:
            @pl.when(me > 0)
            def _():
                if spot[q + 1][1] == 0:
                    halo_copy(slot, spot[q + 1][0], before).wait_recv()
                state_copy(slot, q + 1, before).wait_recv()

            if spot[q + 1][1] == 0:
                take_halo(spot[q + 1][0])

    @pl.when((me > 0) & (step < steps - slots))
    def _():
        pl.semaphore_signal(credit, inc=1, device_id={'sp': before}, device_id_type=pl.DeviceIdType.MESH)

    @pl.when(me == last_device)
    def _():
        n = lax.rem(step, 2)

        @pl.when(step >= 2)
        def _():
            stage_local(n, prompt - 1, layer).wait()
            for k in range(1, devices):
                stage_copy(n, prompt - 1, layer, lax.rem(me + k, devices)).wait_send()

        final = jnp.transpose(s_out_ref[slot])
        for k in range(devices):
            stage_ref[n, k] = final[k * per_device:(k + 1) * per_device, :]
        stage_local(n, prompt, layer).start()
        for k in range(1, devices):
            stage_copy(n, prompt, layer, lax.rem(me + k, devices)).start()

        for j in range(tiles):
            for k in range(3):
                row = k * 2 * 16 + j
                tail_f_ref[pl.ds(layer * 16 + row, 1), :] = u_ref[j, seg + HALO - 3 + k:seg + HALO - 2 + k, :]

        @pl.when(layer == 1)
        def _():
            tail_ref[prompt] = tail_f_ref[...].astype(jnp.bfloat16)

        @pl.when((layer == 1) & (lax.rem(prompt, tail_group) == tail_group - 1))
        def _():
            group = lax.div(prompt, tail_group)
            tail_local(group).start()
            for k in range(1, devices):
                tail_copy(group, lax.rem(me + k, devices)).start()

    for i, rows in enumerate(subs):
        scale = lax.rsqrt(jnp.sum(sum_sq[i], axis=-1, keepdims=True) * (1.0 / d_inner) + EPSILON)
        normed = (g_ref[rows, :] * scale * gate_ref[layer]).astype(jnp.bfloat16)
        res_ref[rows, :] = resid[rows] + dot(normed, w_out_ref[layer])

    @pl.when(layer == 1)
    def _():
        out_ref[0] = res_ref[...]

    @pl.when(step == steps - 1)
    def _():
        @pl.when(me < last_device)
        def _():
            for n in range(slots):
                for group in range(len(groups)):
                    halo_copy(n, group, after).wait_send()
                for q in range(quads):
                    state_copy(n, q, after).wait_send()
            pltpu.make_async_copy(state_hbm, state_hbm, stage_recv).wait()
            pltpu.make_async_copy(tail_hbm, tail_hbm, tail_recv).wait()

        @pl.when(me == last_device)
        def _():
            for n in range(2):
                stage_local(n, batch - 1, n).wait()
                for k in range(1, devices):
                    stage_copy(n, batch - 1, n, lax.rem(me + k, devices)).wait_send()
            for group in range(tail_send.shape[0]):
                tail_local(group).wait()
                for k in range(1, devices):
                    tail_copy(group, lax.rem(me + k, devices)).wait_send()


def solution(mesh):
    seg_count = mesh.shape['sp']

    def forward(resid, pre_norm, w_in, conv_w, conv_b, dt_bias, a_log, d_skip, gate_norm, w_out):
        batch, seg, d_model = resid.shape
        layers, d_inner, _ = w_out.shape
        heads = dt_bias.shape[1]
        head_dim = d_inner // heads
        conv_dim = conv_b.shape[1]
        d_state = (conv_dim - d_inner) // 2
        tiles = conv_dim // LANES
        per_device = d_inner // seg_count
        quads = d_inner // 256
        params = (pre_norm, jnp.swapaxes(conv_w, 1, 2), conv_b, dt_bias, a_log, d_skip, gate_norm)

        def whole(a):
            return pl.BlockSpec(a.shape, lambda p, l: (0,) * a.ndim, pipeline_mode=pl.Buffered(1))

        hbm = pl.BlockSpec(memory_space=pl.ANY)
        block = pl.BlockSpec((1, seg, d_model), lambda p, l: (p, 0, 0))
        out, state, tail = pl.pallas_call(
            functools.partial(forward_kernel, (d_inner, heads, seg, seg_count, batch)),
            grid=(batch, layers),
            out_shape=(jax.ShapeDtypeStruct((batch, seg, d_model), jnp.float32),
                       jax.ShapeDtypeStruct((batch, layers, per_device, d_state), jnp.float32),
                       jax.ShapeDtypeStruct((batch, 6 * 16, LANES), jnp.bfloat16)),
            in_specs=[block, hbm, hbm] + [whole(a) for a in params],
            out_specs=(block, hbm, hbm),
            scratch_shapes=[pltpu.VMEM((seg, d_model), jnp.float32),
                            pltpu.VMEM((layers, d_model, d_inner + conv_dim), jnp.bfloat16),
                            pltpu.VMEM((layers, d_model, LANES), jnp.bfloat16),
                            pltpu.VMEM(w_out.shape, jnp.bfloat16),
                            pltpu.VMEM((2, 256, d_model), jnp.bfloat16),
                            pltpu.VMEM((layers, 8, conv_dim), jnp.float32),
                            pltpu.VMEM((LANES, d_inner), jnp.bfloat16),
                            pltpu.VMEM((tiles, HALO + seg, LANES), jnp.float32),
                            pltpu.VMEM((SLOTS, d_state, d_inner), jnp.float32),
                            pltpu.VMEM((SLOTS, d_state, d_inner), jnp.float32),
                            pltpu.VMEM((SLOTS, 4, 16, LANES), jnp.bfloat16),
                            pltpu.VMEM((SLOTS, 4, 16, LANES), jnp.bfloat16),
                            pltpu.VMEM((2, 4, 16, LANES), jnp.float32),
                            pltpu.VMEM((seg, d_inner), jnp.float32),
                            pltpu.VMEM((2, seg_count, per_device, d_state), jnp.float32),
                            pltpu.VMEM((6 * 16, LANES), jnp.float32),
                            pltpu.VMEM((batch, 6 * 16, LANES), jnp.bfloat16),
                            pltpu.SemaphoreType.DMA((layers,)),
                            pltpu.SemaphoreType.DMA((2,)),
                            pltpu.SemaphoreType.DMA((SLOTS, quads)),
                            pltpu.SemaphoreType.DMA((SLOTS, quads)),
                            pltpu.SemaphoreType.DMA((SLOTS, 4)),
                            pltpu.SemaphoreType.DMA((SLOTS, 4)),
                            pltpu.SemaphoreType.DMA((2, seg_count)),
                            pltpu.SemaphoreType.DMA,
                            pltpu.SemaphoreType.DMA((8, seg_count)),
                            pltpu.SemaphoreType.DMA,
                            pltpu.SemaphoreType.REGULAR],
            compiler_params=pltpu.CompilerParams(dimension_semantics=('arbitrary',) * 2, vmem_limit_bytes=67043328, collective_id=0, has_side_effects=True),
        )(resid, jnp.swapaxes(w_in, 1, 2), w_out, *params)
        tails = tail.reshape(batch, 3, layers, 16, LANES)[:, :, :, :tiles].reshape(batch, 3, layers, conv_dim)
        return out, state.reshape(batch, layers, heads // seg_count, head_dim, d_state), jnp.transpose(tails, (0, 2, 3, 1))

    return jax.shard_map(forward, mesh=mesh, in_specs=(P('dp', 'sp', None), P(), P(), P(), P(), P(), P(), P(), P(), P()), out_specs=(P('dp', 'sp', None), P('dp', None, 'sp', None, None), P('dp', None, None, None)), check_vma=False)
```

```python
import functools

import jax
import jax.numpy as jnp
from jax import lax
from jax.experimental import pallas as pl
from jax.experimental.pallas import tpu as pltpu
from jax.sharding import PartitionSpec as P

EPSILON = 1e-5
HALO = 8
SLOTS = 4
LANES = 128
LOG2_E = 1.4426950408889634


def softplus(v):
    return jnp.maximum(v, 0.0) + jnp.log1p(jnp.exp(-jnp.abs(v)))


def round_bf16(v):
    return v.astype(jnp.bfloat16).astype(jnp.float32)


def dot(a, b):
    return jnp.dot(a, b, preferred_element_type=jnp.float32)


def dot_nt(a, b):
    return lax.dot_general(a, b, (((1,), (1,)), ((), ())), preferred_element_type=jnp.float32)


def forward_kernel(dims, x_ref, w_in_hbm, w_out_hbm, pre_ref, conv_w_ref, conv_b_ref, dt_bias_ref, a_log_ref, d_skip_ref, gate_ref,
                   out_ref, state_hbm, tail_hbm,
                   res_ref, w_in_ref, w_out_ref, row_ref, expand_ref, u_ref, s_in_ref, s_out_ref, halo_in_ref, halo_out_ref, halo_f_ref, g_ref,
                   stage_ref, tail_f_ref, tail_ref,
                   w_sem, raw_sem, s_send, s_recv, halo_send, halo_recv, stage_send, stage_recv, tail_send, tail_recv, credit):
    d_inner, heads, seg, devices, batch = dims
    head_dim = d_inner // heads
    conv_dim = conv_b_ref.shape[1]
    tiles = conv_dim // LANES
    prompt = pl.program_id(0)
    layer = pl.program_id(1)
    me = lax.axis_index('sp')
    quad = 256
    sub = LANES
    quads = d_inner // quad
    bc = quads
    groups = ((bc, 0), (1, 2), (3, 4), (5,))
    spot = {b: (n, 6 * i) for n, group in enumerate(groups) for i, b in enumerate(group)}
    steps = batch * 2
    step = prompt * 2 + layer
    slots = s_in_ref.shape[0]
    slot = lax.rem(step, slots)
    last_device = devices - 1
    after = lax.rem(me + 1, devices)
    before = lax.rem(me + devices - 1, devices)
    tail_group = batch // tail_send.shape[0]
    per_device = d_inner // devices

    def w_in_copy(l):
        rows = pl.ds(0, w_in_hbm.shape[1])
        return pltpu.make_async_copy(w_in_hbm.at[l], w_in_ref.at[l, rows, :], raw_sem.at[l])

    def w_out_copy(l):
        return pltpu.make_async_copy(w_out_hbm.at[l], w_out_ref.at[l], w_sem.at[l])

    def remote(src, dst, send, recv, peer):
        return pltpu.make_async_remote_copy(src_ref=src, dst_ref=dst, send_sem=send, recv_sem=recv, device_id={'sp': peer},
                                            device_id_type=pl.DeviceIdType.MESH)

    def state_copy(n, q, peer):
        cols = pl.ds(q * quad, quad)
        return remote(s_out_ref.at[n, :, cols], s_in_ref.at[n, :, cols], s_send.at[n, q], s_recv.at[n, q], peer)

    def halo_copy(n, group, peer):
        return remote(halo_out_ref.at[n, group], halo_in_ref.at[n, group], halo_send.at[n, group], halo_recv.at[n, group], peer)

    def stage_copy(n, p, l, peer):
        return remote(stage_ref.at[n, peer], state_hbm.at[p, l], stage_send.at[n, peer], stage_recv, peer)

    def stage_local(n, p, l):
        return pltpu.make_async_copy(stage_ref.at[n, me], state_hbm.at[p, l], stage_send.at[n, me])

    def tail_copy(group, peer):
        rows = pl.ds(group * tail_group, tail_group)
        return remote(tail_ref.at[rows], tail_hbm.at[rows], tail_send.at[group, peer], tail_recv, peer)

    def tail_local(group):
        rows = pl.ds(group * tail_group, tail_group)
        return pltpu.make_async_copy(tail_ref.at[rows], tail_hbm.at[rows], tail_send.at[group, me])

    left = lax.broadcasted_iota(jnp.int32, (sub, LANES), 1) < head_dim

    @pl.when(step == 0)
    def _():
        for l in range(2):
            w_in_copy(l).start()
            w_out_copy(l).start()
        barrier = pltpu.get_barrier_semaphore()
        for k in range(1, devices):
            pl.semaphore_signal(barrier, inc=1, device_id={'sp': lax.rem(me + k, devices)}, device_id_type=pl.DeviceIdType.MESH)

        tail_f_ref[...] = jnp.zeros(tail_f_ref.shape, jnp.float32)
        halo_f_ref[...] = jnp.zeros(halo_f_ref.shape, jnp.float32)
        row_ref[...] = jnp.zeros(row_ref.shape, jnp.float32)

        @pl.when(me == 0)
        def _():
            s_in_ref[...] = jnp.zeros(s_in_ref.shape, jnp.float32)
            halo_in_ref[...] = jnp.zeros(halo_in_ref.shape, jnp.bfloat16)

        for l in range(2):
            for tap in range(4):
                row_ref[l, tap:tap + 1, 0:conv_dim] = 0.5 * conv_w_ref[l, tap:tap + 1, :]
            row_ref[l, 4:5, 0:conv_dim] = 0.5 * conv_b_ref[l:l + 1, :]
            row_ref[l, 5:6, 0:heads] = dt_bias_ref[l:l + 1, :]
            row_ref[l, 6:7, 0:heads] = -jnp.exp(a_log_ref[l:l + 1, :]) * LOG2_E
            for k in range(d_inner // LANES):
                d_left = jnp.broadcast_to(d_skip_ref[l:l + 1, 2 * k:2 * k + 1], (1, LANES))
                d_right = jnp.broadcast_to(d_skip_ref[l:l + 1, 2 * k + 1:2 * k + 2], (1, LANES))
                row_ref[l, 7:8, k * LANES:(k + 1) * LANES] = jnp.where(left[0:1], d_left, d_right)
        lane_head = lax.shift_right_logical(lax.broadcasted_iota(jnp.int32, expand_ref.shape, 1), 6)
        expand_ref[...] = jnp.where(lax.broadcasted_iota(jnp.int32, expand_ref.shape, 0) == lane_head, 1.0, 0.0).astype(jnp.bfloat16)

        pl.semaphore_wait(barrier, devices - 1)

    @pl.when(prompt == 0)
    def _():
        w_in_copy(layer).wait()
        w_out_copy(layer).wait()
        w_in_ref[layer, w_in_hbm.shape[1]:, :] = jnp.zeros((w_in_ref.shape[1] - w_in_hbm.shape[1], w_in_ref.shape[2]), jnp.bfloat16)

    @pl.when((me < last_device) & (step >= slots))
    def _():
        for n in range(len(groups)):
            halo_copy(slot, n, after).wait_send()
        for q in range(quads):
            state_copy(slot, q, after).wait_send()
        pl.semaphore_wait(credit, 1)

    @pl.when(layer == 0)
    def _():
        res_ref[...] = x_ref[0]

    resid = res_ref[...]
    mean_sq = jnp.mean(resid * resid, axis=-1, keepdims=True)
    h = (resid * lax.rsqrt(mean_sq + EPSILON) * pre_ref[pl.ds(layer, 1), :]).astype(jnp.bfloat16)

    def project(b):
        first_col = b * quad
        u = round_bf16(dot_nt(h, w_in_ref[layer, d_inner + first_col:d_inner + first_col + quad, :]))
        for k in range(quad // LANES):
            j = first_col // LANES + k
            lanes = slice(k * LANES, (k + 1) * LANES)
            u_ref[j, HALO:HALO + seg, :] = u[:, lanes]
            group, first = spot[b]
            for tap in range(3):
                row = first + 2 * tap + k
                halo_f_ref[0, group, row:row + 1, :] = u_ref[j, HALO + seg - 3 + tap:HALO + seg - 2 + tap, :]

    def project_group(group):
        for b in groups[group]:
            project(b)
        halo_out_ref[slot, group] = halo_f_ref[0, group].astype(jnp.bfloat16)

    def take_halo(group):
        halo_f_ref[1, group] = halo_in_ref[slot, group].astype(jnp.float32)

    def conv(b):
        outs = []
        for j in range(b * quad // LANES, (b + 1) * quad // LANES):
            cols = slice(j * LANES, (j + 1) * LANES)
            group, first = spot[b]
            for tap in range(3):
                row = first + 2 * tap + j % 2
                u_ref[j, HALO - 3 + tap:HALO - 2 + tap, :] = halo_f_ref[1, group, row:row + 1, :]
            acc = row_ref[layer, 4:5, cols]
            for tap in range(4):
                acc = acc + u_ref[j, HALO - 3 + tap:HALO - 3 + tap + seg, :] * row_ref[layer, tap:tap + 1, cols]
            outs.append((acc + acc * jnp.tanh(acc)).astype(jnp.bfloat16))
        return outs

    dt_raw = round_bf16(dot_nt(h, w_in_ref[layer, d_inner + conv_dim:d_inner + conv_dim + LANES, :]))
    delta = softplus(dt_raw + row_ref[layer, 5:6, 0:LANES]).astype(jnp.bfloat16)
    project_group(0)

    @pl.when(me < last_device)
    def _():
        halo_copy(slot, 0, after).start()

    @pl.when(me > 0)
    def _():
        halo_copy(slot, 0, before).wait_recv()

    take_halo(0)
    b_act, c_act = conv(bc)
    causal = lax.broadcasted_iota(jnp.int32, (sub, sub), 0) >= lax.broadcasted_iota(jnp.int32, (sub, sub), 1)
    tri = jnp.where(causal, 1.0, 0.0).astype(jnp.bfloat16)
    b_t = jnp.transpose(b_act.astype(jnp.float32)).astype(jnp.bfloat16)
    subs = [slice(i * sub, (i + 1) * sub) for i in range(seg // sub)]
    cums = [dot(tri, delta[rows]) * row_ref[layer, 6:7, 0:LANES] for rows in subs]
    cums_t = [jnp.transpose(cum) for cum in cums]
    scores = [jnp.where(causal, dot_nt(c_act[rows], b_act[rows]), 0.0) for rows in subs]

    def local_part(q):
        cols = slice(q * quad, (q + 1) * quad)
        x_tiles = conv(q)
        if q + 1 < len(groups):
            project_group(q + 1)
        z = dot_nt(h, w_in_ref[layer, cols, :]).astype(jnp.bfloat16)
        dt_wide = dot(delta, expand_ref[:, cols])
        parts = []
        for i, rows in enumerate(subs):
            x_ends = []
            decays = []
            ys = []
            scales = []
            for k in range(quad // LANES):
                lanes = slice(k * LANES, (k + 1) * LANES)
                head = (q * quad + k * LANES) // head_dim
                x_float = x_tiles[k][rows].astype(jnp.float32)
                x_scaled = x_float * dt_wide[rows, lanes]
                x_dot = x_scaled.astype(jnp.bfloat16)
                wide = [jnp.broadcast_to(cums[i][:, head + n:head + n + 1], (sub, LANES)) for n in range(2)]
                mix = [(jnp.exp2(jnp.minimum(wide[n] - cums_t[i][head + n:head + n + 1, :], 0.0)) * scores[i]).astype(jnp.bfloat16) for n in range(2)]
                none = jnp.zeros_like(x_dot)
                pair_rhs = jnp.concatenate([jnp.where(left, x_dot, none), jnp.where(left, none, x_dot)], axis=0)
                y_intra = dot(jnp.concatenate(mix, axis=1), pair_rhs)
                cum_pair = jnp.where(left, wide[0], wide[1])
                last = cum_pair[sub - 1:sub, :]
                x_ends.append((x_scaled * jnp.exp2(last - cum_pair)).astype(jnp.bfloat16))
                decays.append(jnp.exp2(last))
                tile = slice(q * quad + k * LANES, q * quad + (k + 1) * LANES)
                ys.append(y_intra + row_ref[layer, 7:8, tile] * x_float)
                scales.append(jnp.exp2(cum_pair))
            added = dot(b_t[:, rows], jnp.concatenate(x_ends, axis=1))
            parts.append((jnp.concatenate(decays, axis=1), added, ys, scales))
        return z, parts

    def gate_part(q, z, parts, states, sums):
        for i, rows in enumerate(subs):
            y_inter = dot(c_act[rows], states[i].astype(jnp.bfloat16))
            for k in range(quad // LANES):
                lanes = slice(k * LANES, (k + 1) * LANES)
                y = parts[i][2][k] + y_inter[:, lanes] * parts[i][3][k]
                z_half = 0.5 * z[rows, lanes].astype(jnp.float32)
                gated = round_bf16(y) * (z_half + z_half * jnp.tanh(z_half))
                g_ref[rows, q * quad + k * LANES:q * quad + (k + 1) * LANES] = gated
                sums[i] = sums[i] + gated * gated

    sum_sq = [jnp.zeros((sub, LANES), jnp.float32) for _ in subs]
    z, parts = local_part(0)
    for q in range(quads):
        cols = slice(q * quad, (q + 1) * quad)

        @pl.when(me < last_device)
        def _():
            if q + 1 < len(groups):
                halo_copy(slot, q + 1, after).start()

        @pl.when(me > 0)
        def _():
            state_copy(slot, q, before).wait_recv()

        states = [s_in_ref[slot, :, cols]]
        for decay, added, _, _ in parts:
            states.append(states[-1] * decay + added)
        s_out_ref[slot, :, cols] = states[-1]

        @pl.when(me < last_device)
        def _():
            state_copy(slot, q, after).start()

        if q + 1 < quads and spot[q + 1][1] == 0:
            @pl.when(me > 0)
            def _():
                halo_copy(slot, spot[q + 1][0], before).wait_recv()

            take_halo(spot[q + 1][0])
        gate_part(q, z, parts, states, sum_sq)
        if q + 1 < quads:
            z, parts = local_part(q + 1)

    @pl.when((me > 0) & (step < steps - slots))
    def _():
        pl.semaphore_signal(credit, inc=1, device_id={'sp': before}, device_id_type=pl.DeviceIdType.MESH)

    @pl.when(me == last_device)
    def _():
        n = lax.rem(step, 2)

        @pl.when(step >= 2)
        def _():
            stage_local(n, prompt - 1, layer).wait()
            for k in range(1, devices):
                stage_copy(n, prompt - 1, layer, lax.rem(me + k, devices)).wait_send()

        final = jnp.transpose(s_out_ref[slot])
        for k in range(devices):
            stage_ref[n, k] = final[k * per_device:(k + 1) * per_device, :]
        stage_local(n, prompt, layer).start()
        for k in range(1, devices):
            stage_copy(n, prompt, layer, lax.rem(me + k, devices)).start()

        for j in range(tiles):
            for k in range(3):
                row = k * 2 * 16 + j
                tail_f_ref[pl.ds(layer * 16 + row, 1), :] = u_ref[j, seg + HALO - 3 + k:seg + HALO - 2 + k, :]

        @pl.when(layer == 1)
        def _():
            tail_ref[prompt] = tail_f_ref[...].astype(jnp.bfloat16)

        @pl.when((layer == 1) & (lax.rem(prompt, tail_group) == tail_group - 1))
        def _():
            group = lax.div(prompt, tail_group)
            tail_local(group).start()
            for k in range(1, devices):
                tail_copy(group, lax.rem(me + k, devices)).start()

    for i, rows in enumerate(subs):
        scale = lax.rsqrt(jnp.sum(sum_sq[i], axis=-1, keepdims=True) * (1.0 / d_inner) + EPSILON)
        normed = (g_ref[rows, :] * scale * gate_ref[layer]).astype(jnp.bfloat16)
        res_ref[rows, :] = resid[rows] + dot(normed, w_out_ref[layer])

    @pl.when(layer == 1)
    def _():
        out_ref[0] = res_ref[...]

    @pl.when(step == steps - 1)
    def _():
        @pl.when(me < last_device)
        def _():
            for n in range(slots):
                for group in range(len(groups)):
                    halo_copy(n, group, after).wait_send()
                for q in range(quads):
                    state_copy(n, q, after).wait_send()
            pltpu.make_async_copy(state_hbm, state_hbm, stage_recv).wait()
            pltpu.make_async_copy(tail_hbm, tail_hbm, tail_recv).wait()

        @pl.when(me == last_device)
        def _():
            for n in range(2):
                stage_local(n, batch - 1, n).wait()
                for k in range(1, devices):
                    stage_copy(n, batch - 1, n, lax.rem(me + k, devices)).wait_send()
            for group in range(tail_send.shape[0]):
                tail_local(group).wait()
                for k in range(1, devices):
                    tail_copy(group, lax.rem(me + k, devices)).wait_send()


def solution(mesh):
    seg_count = mesh.shape['sp']

    def forward(resid, pre_norm, w_in, conv_w, conv_b, dt_bias, a_log, d_skip, gate_norm, w_out):
        batch, seg, d_model = resid.shape
        layers, d_inner, _ = w_out.shape
        heads = dt_bias.shape[1]
        head_dim = d_inner // heads
        conv_dim = conv_b.shape[1]
        d_state = (conv_dim - d_inner) // 2
        tiles = conv_dim // LANES
        per_device = d_inner // seg_count
        quads = d_inner // 256
        params = (pre_norm, jnp.swapaxes(conv_w, 1, 2), conv_b, dt_bias, a_log, d_skip, gate_norm)

        def whole(a):
            return pl.BlockSpec(a.shape, lambda p, l: (0,) * a.ndim, pipeline_mode=pl.Buffered(1))

        hbm = pl.BlockSpec(memory_space=pl.ANY)
        block = pl.BlockSpec((1, seg, d_model), lambda p, l: (p, 0, 0))
        out, state, tail = pl.pallas_call(
            functools.partial(forward_kernel, (d_inner, heads, seg, seg_count, batch)),
            grid=(batch, layers),
            out_shape=(jax.ShapeDtypeStruct((batch, seg, d_model), jnp.float32),
                       jax.ShapeDtypeStruct((batch, layers, per_device, d_state), jnp.float32),
                       jax.ShapeDtypeStruct((batch, 6 * 16, LANES), jnp.bfloat16)),
            in_specs=[block, hbm, hbm] + [whole(a) for a in params],
            out_specs=(block, hbm, hbm),
            scratch_shapes=[pltpu.VMEM((seg, d_model), jnp.float32),
                            pltpu.VMEM((layers, d_inner + conv_dim + LANES, d_model), jnp.bfloat16),
                            pltpu.VMEM(w_out.shape, jnp.bfloat16),
                            pltpu.VMEM((layers, 8, conv_dim), jnp.float32),
                            pltpu.VMEM((LANES, d_inner), jnp.bfloat16),
                            pltpu.VMEM((tiles, HALO + seg, LANES), jnp.float32),
                            pltpu.VMEM((SLOTS, d_state, d_inner), jnp.float32),
                            pltpu.VMEM((SLOTS, d_state, d_inner), jnp.float32),
                            pltpu.VMEM((SLOTS, 4, 16, LANES), jnp.bfloat16),
                            pltpu.VMEM((SLOTS, 4, 16, LANES), jnp.bfloat16),
                            pltpu.VMEM((2, 4, 16, LANES), jnp.float32),
                            pltpu.VMEM((seg, d_inner), jnp.float32),
                            pltpu.VMEM((2, seg_count, per_device, d_state), jnp.float32),
                            pltpu.VMEM((6 * 16, LANES), jnp.float32),
                            pltpu.VMEM((batch, 6 * 16, LANES), jnp.bfloat16),
                            pltpu.SemaphoreType.DMA((layers,)),
                            pltpu.SemaphoreType.DMA((2,)),
                            pltpu.SemaphoreType.DMA((SLOTS, quads)),
                            pltpu.SemaphoreType.DMA((SLOTS, quads)),
                            pltpu.SemaphoreType.DMA((SLOTS, 4)),
                            pltpu.SemaphoreType.DMA((SLOTS, 4)),
                            pltpu.SemaphoreType.DMA((2, seg_count)),
                            pltpu.SemaphoreType.DMA,
                            pltpu.SemaphoreType.DMA((8, seg_count)),
                            pltpu.SemaphoreType.DMA,
                            pltpu.SemaphoreType.REGULAR],
            compiler_params=pltpu.CompilerParams(dimension_semantics=('arbitrary',) * 2, vmem_limit_bytes=67043328, collective_id=0, has_side_effects=True),
        )(resid, jnp.swapaxes(w_in, 1, 2), w_out, *params)
        tails = tail.reshape(batch, 3, layers, 16, LANES)[:, :, :, :tiles].reshape(batch, 3, layers, conv_dim)
        return out, state.reshape(batch, layers, heads // seg_count, head_dim, d_state), jnp.transpose(tails, (0, 2, 3, 1))

    return jax.shard_map(forward, mesh=mesh, in_specs=(P('dp', 'sp', None), P(), P(), P(), P(), P(), P(), P(), P(), P()), out_specs=(P('dp', 'sp', None), P('dp', None, 'sp', None, None), P('dp', None, None, None)), check_vma=False)
```

```python
import functools

import jax
import jax.numpy as jnp
from jax import lax
from jax.experimental import pallas as pl
from jax.experimental.pallas import tpu as pltpu
from jax.sharding import PartitionSpec as P

EPSILON = 1e-5
HALO = 8
SLOTS = 4
LANES = 128
LOG2_E = 1.4426950408889634


def softplus(v):
    return jnp.maximum(v, 0.0) + jnp.log1p(jnp.exp(-jnp.abs(v)))


def round_bf16(v):
    return v.astype(jnp.bfloat16).astype(jnp.float32)


def dot(a, b):
    return jnp.dot(a, b, preferred_element_type=jnp.float32)


def dot_nt(a, b):
    return lax.dot_general(a, b, (((1,), (1,)), ((), ())), preferred_element_type=jnp.float32)


def forward_kernel(dims, x_ref, w_in_hbm, w_out_hbm, pre_ref, conv_w_ref, conv_b_ref, dt_bias_ref, a_log_ref, d_skip_ref, gate_ref,
                   out_ref, state_hbm, tail_hbm,
                   res_ref, w_in_ref, w_out_ref, row_ref, expand_ref, u_ref, s_in_ref, s_out_ref, halo_in_ref, halo_out_ref, halo_f_ref, g_ref,
                   stage_ref, tail_f_ref, tail_ref,
                   w_sem, raw_sem, s_send, s_recv, halo_send, halo_recv, stage_send, stage_recv, tail_send, tail_recv, credit):
    d_inner, heads, seg, devices, batch = dims
    head_dim = d_inner // heads
    conv_dim = conv_b_ref.shape[1]
    tiles = conv_dim // LANES
    prompt = pl.program_id(0)
    layer = pl.program_id(1)
    me = lax.axis_index('sp')
    quad = 256
    sub = LANES
    quads = d_inner // quad
    bc = quads
    groups = ((bc, 0), tuple(range(1, quads)))
    spans = ((0, 16), (16, 32))
    spot = {b: (n, spans[n][0] + 6 * i) for n, group in enumerate(groups) for i, b in enumerate(group)}
    steps = batch * 2
    step = prompt * 2 + layer
    slots = s_in_ref.shape[0]
    slot = lax.rem(step, slots)
    last_device = devices - 1
    after = lax.rem(me + 1, devices)
    before = lax.rem(me + devices - 1, devices)
    tail_group = batch // tail_send.shape[0]
    per_device = d_inner // devices

    def w_in_copy(l):
        rows = pl.ds(0, w_in_hbm.shape[1])
        return pltpu.make_async_copy(w_in_hbm.at[l], w_in_ref.at[l, rows, :], raw_sem.at[l])

    def w_out_copy(l):
        return pltpu.make_async_copy(w_out_hbm.at[l], w_out_ref.at[l], w_sem.at[l])

    def remote(src, dst, send, recv, peer):
        return pltpu.make_async_remote_copy(src_ref=src, dst_ref=dst, send_sem=send, recv_sem=recv, device_id={'sp': peer},
                                            device_id_type=pl.DeviceIdType.MESH)

    def state_copy(n, q, peer):
        cols = pl.ds(q * quad, quad)
        return remote(s_out_ref.at[n, :, cols], s_in_ref.at[n, :, cols], s_send.at[n, q], s_recv.at[n, q], peer)

    def halo_copy(n, group, peer):
        rows = pl.ds(*spans[group])
        return remote(halo_out_ref.at[n, rows], halo_in_ref.at[n, rows], halo_send.at[n, group], halo_recv.at[n, group], peer)

    def stage_copy(n, p, l, peer):
        return remote(stage_ref.at[n, peer], state_hbm.at[p, l], stage_send.at[n, peer], stage_recv, peer)

    def stage_local(n, p, l):
        return pltpu.make_async_copy(stage_ref.at[n, me], state_hbm.at[p, l], stage_send.at[n, me])

    def tail_copy(group, peer):
        rows = pl.ds(group * tail_group, tail_group)
        return remote(tail_ref.at[rows], tail_hbm.at[rows], tail_send.at[group, peer], tail_recv, peer)

    def tail_local(group):
        rows = pl.ds(group * tail_group, tail_group)
        return pltpu.make_async_copy(tail_ref.at[rows], tail_hbm.at[rows], tail_send.at[group, me])

    left = lax.broadcasted_iota(jnp.int32, (sub, LANES), 1) < head_dim

    @pl.when(step == 0)
    def _():
        for l in range(2):
            w_in_copy(l).start()
            w_out_copy(l).start()
        barrier = pltpu.get_barrier_semaphore()
        for k in range(1, devices):
            pl.semaphore_signal(barrier, inc=1, device_id={'sp': lax.rem(me + k, devices)}, device_id_type=pl.DeviceIdType.MESH)

        tail_f_ref[...] = jnp.zeros(tail_f_ref.shape, jnp.float32)
        halo_f_ref[...] = jnp.zeros(halo_f_ref.shape, jnp.float32)
        row_ref[...] = jnp.zeros(row_ref.shape, jnp.float32)

        @pl.when(me == 0)
        def _():
            s_in_ref[...] = jnp.zeros(s_in_ref.shape, jnp.float32)
            halo_in_ref[...] = jnp.zeros(halo_in_ref.shape, jnp.bfloat16)

        for l in range(2):
            for tap in range(4):
                row_ref[l, tap:tap + 1, 0:conv_dim] = 0.5 * conv_w_ref[l, tap:tap + 1, :]
            row_ref[l, 4:5, 0:conv_dim] = 0.5 * conv_b_ref[l:l + 1, :]
            row_ref[l, 5:6, 0:heads] = dt_bias_ref[l:l + 1, :]
            row_ref[l, 6:7, 0:heads] = -jnp.exp(a_log_ref[l:l + 1, :]) * LOG2_E
            for k in range(d_inner // LANES):
                d_left = jnp.broadcast_to(d_skip_ref[l:l + 1, 2 * k:2 * k + 1], (1, LANES))
                d_right = jnp.broadcast_to(d_skip_ref[l:l + 1, 2 * k + 1:2 * k + 2], (1, LANES))
                row_ref[l, 7:8, k * LANES:(k + 1) * LANES] = jnp.where(left[0:1], d_left, d_right)
        lane_head = lax.shift_right_logical(lax.broadcasted_iota(jnp.int32, expand_ref.shape, 1), 6)
        expand_ref[...] = jnp.where(lax.broadcasted_iota(jnp.int32, expand_ref.shape, 0) == lane_head, 1.0, 0.0).astype(jnp.bfloat16)

        pl.semaphore_wait(barrier, devices - 1)

    @pl.when(prompt == 0)
    def _():
        w_in_copy(layer).wait()
        w_out_copy(layer).wait()
        w_in_ref[layer, w_in_hbm.shape[1]:, :] = jnp.zeros((w_in_ref.shape[1] - w_in_hbm.shape[1], w_in_ref.shape[2]), jnp.bfloat16)

    @pl.when((me < last_device) & (step >= slots))
    def _():
        for n in range(len(groups)):
            halo_copy(slot, n, after).wait_send()
        for q in range(quads):
            state_copy(slot, q, after).wait_send()
        pl.semaphore_wait(credit, 1)

    @pl.when(layer == 0)
    def _():
        res_ref[...] = x_ref[0]

    resid = res_ref[...]
    mean_sq = jnp.mean(resid * resid, axis=-1, keepdims=True)
    h = (resid * lax.rsqrt(mean_sq + EPSILON) * pre_ref[pl.ds(layer, 1), :]).astype(jnp.bfloat16)

    def project(b):
        first_col = b * quad
        u = round_bf16(dot_nt(h, w_in_ref[layer, d_inner + first_col:d_inner + first_col + quad, :]))
        for k in range(quad // LANES):
            j = first_col // LANES + k
            lanes = slice(k * LANES, (k + 1) * LANES)
            u_ref[j, HALO:HALO + seg, :] = u[:, lanes]
            group, first = spot[b]
            for tap in range(3):
                row = first + 2 * tap + k
                halo_f_ref[0, row:row + 1, :] = u_ref[j, HALO + seg - 3 + tap:HALO + seg - 2 + tap, :]

    def project_group(group):
        for b in groups[group]:
            project(b)
        first, count = spans[group]
        halo_out_ref[slot, first:first + count, :] = halo_f_ref[0, first:first + count, :].astype(jnp.bfloat16)

    def take_halo(group):
        first, count = spans[group]
        halo_f_ref[1, first:first + count, :] = halo_in_ref[slot, first:first + count, :].astype(jnp.float32)

    def conv(b):
        outs = []
        for j in range(b * quad // LANES, (b + 1) * quad // LANES):
            cols = slice(j * LANES, (j + 1) * LANES)
            group, first = spot[b]
            for tap in range(3):
                row = first + 2 * tap + j % 2
                u_ref[j, HALO - 3 + tap:HALO - 2 + tap, :] = halo_f_ref[1, row:row + 1, :]
            acc = row_ref[layer, 4:5, cols]
            for tap in range(4):
                acc = acc + u_ref[j, HALO - 3 + tap:HALO - 3 + tap + seg, :] * row_ref[layer, tap:tap + 1, cols]
            outs.append((acc + acc * jnp.tanh(acc)).astype(jnp.bfloat16))
        return outs

    dt_raw = round_bf16(dot_nt(h, w_in_ref[layer, d_inner + conv_dim:d_inner + conv_dim + LANES, :]))
    delta = softplus(dt_raw + row_ref[layer, 5:6, 0:LANES]).astype(jnp.bfloat16)
    project_group(0)

    @pl.when(me < last_device)
    def _():
        halo_copy(slot, 0, after).start()

    @pl.when(me > 0)
    def _():
        halo_copy(slot, 0, before).wait_recv()

    take_halo(0)
    b_act, c_act = conv(bc)
    causal = lax.broadcasted_iota(jnp.int32, (sub, sub), 0) >= lax.broadcasted_iota(jnp.int32, (sub, sub), 1)
    tri = jnp.where(causal, 1.0, 0.0).astype(jnp.bfloat16)
    b_t = jnp.transpose(b_act.astype(jnp.float32)).astype(jnp.bfloat16)
    subs = [slice(i * sub, (i + 1) * sub) for i in range(seg // sub)]
    cums = [dot(tri, delta[rows]) * row_ref[layer, 6:7, 0:LANES] for rows in subs]
    cums_t = [jnp.transpose(cum) for cum in cums]
    scores = [jnp.where(causal, dot_nt(c_act[rows], b_act[rows]), 0.0) for rows in subs]

    def local_part(q):
        cols = slice(q * quad, (q + 1) * quad)
        x_tiles = conv(q)
        if q + 1 < len(groups):
            project_group(q + 1)
        z = dot_nt(h, w_in_ref[layer, cols, :]).astype(jnp.bfloat16)
        dt_wide = dot(delta, expand_ref[:, cols])
        parts = []
        for i, rows in enumerate(subs):
            x_ends = []
            decays = []
            ys = []
            scales = []
            for k in range(quad // LANES):
                lanes = slice(k * LANES, (k + 1) * LANES)
                head = (q * quad + k * LANES) // head_dim
                x_float = x_tiles[k][rows].astype(jnp.float32)
                x_scaled = x_float * dt_wide[rows, lanes]
                x_dot = x_scaled.astype(jnp.bfloat16)
                wide = [jnp.broadcast_to(cums[i][:, head + n:head + n + 1], (sub, LANES)) for n in range(2)]
                mix = [(jnp.exp2(jnp.minimum(wide[n] - cums_t[i][head + n:head + n + 1, :], 0.0)) * scores[i]).astype(jnp.bfloat16) for n in range(2)]
                none = jnp.zeros_like(x_dot)
                pair_rhs = jnp.concatenate([jnp.where(left, x_dot, none), jnp.where(left, none, x_dot)], axis=0)
                y_intra = dot(jnp.concatenate(mix, axis=1), pair_rhs)
                cum_pair = jnp.where(left, wide[0], wide[1])
                last = cum_pair[sub - 1:sub, :]
                x_ends.append((x_scaled * jnp.exp2(last - cum_pair)).astype(jnp.bfloat16))
                decays.append(jnp.exp2(last))
                tile = slice(q * quad + k * LANES, q * quad + (k + 1) * LANES)
                ys.append(y_intra + row_ref[layer, 7:8, tile] * x_float)
                scales.append(jnp.exp2(cum_pair))
            added = dot(b_t[:, rows], jnp.concatenate(x_ends, axis=1))
            parts.append((jnp.concatenate(decays, axis=1), added, ys, scales))
        return z, parts

    def gate_part(q, z, parts, states, sums):
        for i, rows in enumerate(subs):
            y_inter = dot(c_act[rows], states[i].astype(jnp.bfloat16))
            for k in range(quad // LANES):
                lanes = slice(k * LANES, (k + 1) * LANES)
                y = parts[i][2][k] + y_inter[:, lanes] * parts[i][3][k]
                z_half = 0.5 * z[rows, lanes].astype(jnp.float32)
                gated = round_bf16(y) * (z_half + z_half * jnp.tanh(z_half))
                g_ref[rows, q * quad + k * LANES:q * quad + (k + 1) * LANES] = gated
                sums[i] = sums[i] + gated * gated

    sum_sq = [jnp.zeros((sub, LANES), jnp.float32) for _ in subs]
    z, parts = local_part(0)
    for q in range(quads):
        cols = slice(q * quad, (q + 1) * quad)

        @pl.when(me < last_device)
        def _():
            if q + 1 < len(groups):
                halo_copy(slot, q + 1, after).start()

        @pl.when(me > 0)
        def _():
            state_copy(slot, q, before).wait_recv()

        states = [s_in_ref[slot, :, cols]]
        for decay, added, _, _ in parts:
            states.append(states[-1] * decay + added)
        s_out_ref[slot, :, cols] = states[-1]

        @pl.when(me < last_device)
        def _():
            state_copy(slot, q, after).start()

        if q == 0:
            @pl.when(me > 0)
            def _():
                halo_copy(slot, 1, before).wait_recv()

            take_halo(1)
        gate_part(q, z, parts, states, sum_sq)
        if q + 1 < quads:
            z, parts = local_part(q + 1)

    @pl.when((me > 0) & (step < steps - slots))
    def _():
        pl.semaphore_signal(credit, inc=1, device_id={'sp': before}, device_id_type=pl.DeviceIdType.MESH)

    @pl.when(me == last_device)
    def _():
        n = lax.rem(step, 2)

        @pl.when(step >= 2)
        def _():
            stage_local(n, prompt - 1, layer).wait()
            for k in range(1, devices):
                stage_copy(n, prompt - 1, layer, lax.rem(me + k, devices)).wait_send()

        final = jnp.transpose(s_out_ref[slot])
        for k in range(devices):
            stage_ref[n, k] = final[k * per_device:(k + 1) * per_device, :]
        stage_local(n, prompt, layer).start()
        for k in range(1, devices):
            stage_copy(n, prompt, layer, lax.rem(me + k, devices)).start()

        for l in range(2):
            @pl.when(layer == l)
            def _():
                for j in range(tiles):
                    for k in range(3):
                        tail_f_ref[k, l:l + 1, j * LANES:(j + 1) * LANES] = u_ref[j, seg + HALO - 3 + k:seg + HALO - 2 + k, :]

        @pl.when(layer == 1)
        def _():
            tail_ref[prompt] = tail_f_ref[...].astype(jnp.bfloat16)

        @pl.when((layer == 1) & (lax.rem(prompt, tail_group) == tail_group - 1))
        def _():
            group = lax.div(prompt, tail_group)
            tail_local(group).start()
            for k in range(1, devices):
                tail_copy(group, lax.rem(me + k, devices)).start()

    for i, rows in enumerate(subs):
        scale = lax.rsqrt(jnp.sum(sum_sq[i], axis=-1, keepdims=True) * (1.0 / d_inner) + EPSILON)
        normed = (g_ref[rows, :] * scale * gate_ref[layer]).astype(jnp.bfloat16)
        res_ref[rows, :] = resid[rows] + dot(normed, w_out_ref[layer])

    @pl.when(layer == 1)
    def _():
        out_ref[0] = res_ref[...]

    @pl.when(step == steps - 1)
    def _():
        @pl.when(me < last_device)
        def _():
            for n in range(slots):
                for group in range(len(groups)):
                    halo_copy(n, group, after).wait_send()
                for q in range(quads):
                    state_copy(n, q, after).wait_send()
            pltpu.make_async_copy(state_hbm, state_hbm, stage_recv).wait()
            pltpu.make_async_copy(tail_hbm, tail_hbm, tail_recv).wait()

        @pl.when(me == last_device)
        def _():
            for n in range(2):
                stage_local(n, batch - 1, n).wait()
                for k in range(1, devices):
                    stage_copy(n, batch - 1, n, lax.rem(me + k, devices)).wait_send()
            @pl.loop(0, tail_send.shape[0])
            def _(group):
                tail_local(group).wait()
                for k in range(1, devices):
                    tail_copy(group, lax.rem(me + k, devices)).wait_send()


def solution(mesh):
    seg_count = mesh.shape['sp']

    def forward(resid, pre_norm, w_in, conv_w, conv_b, dt_bias, a_log, d_skip, gate_norm, w_out):
        batch, seg, d_model = resid.shape
        layers, d_inner, _ = w_out.shape
        heads = dt_bias.shape[1]
        head_dim = d_inner // heads
        conv_dim = conv_b.shape[1]
        d_state = (conv_dim - d_inner) // 2
        tiles = conv_dim // LANES
        per_device = d_inner // seg_count
        quads = d_inner // 256
        params = (pre_norm, jnp.swapaxes(conv_w, 1, 2), conv_b, dt_bias, a_log, d_skip, gate_norm)

        def whole(a):
            return pl.BlockSpec(a.shape, lambda p, l: (0,) * a.ndim, pipeline_mode=pl.Buffered(1))

        hbm = pl.BlockSpec(memory_space=pl.ANY)
        block = pl.BlockSpec((1, seg, d_model), lambda p, l: (p, 0, 0))
        out, state, tail = pl.pallas_call(
            functools.partial(forward_kernel, (d_inner, heads, seg, seg_count, batch)),
            grid=(batch, layers),
            out_shape=(jax.ShapeDtypeStruct((batch, seg, d_model), jnp.float32),
                       jax.ShapeDtypeStruct((batch, layers, per_device, d_state), jnp.float32),
                       jax.ShapeDtypeStruct((batch, 3, layers, conv_dim), jnp.bfloat16)),
            in_specs=[block, hbm, hbm] + [whole(a) for a in params],
            out_specs=(block, hbm, hbm),
            scratch_shapes=[pltpu.VMEM((seg, d_model), jnp.float32),
                            pltpu.VMEM((layers, d_inner + conv_dim + LANES, d_model), jnp.bfloat16),
                            pltpu.VMEM(w_out.shape, jnp.bfloat16),
                            pltpu.VMEM((layers, 8, conv_dim), jnp.float32),
                            pltpu.VMEM((LANES, d_inner), jnp.bfloat16),
                            pltpu.VMEM((tiles, HALO + seg, LANES), jnp.float32),
                            pltpu.VMEM((SLOTS, d_state, d_inner), jnp.float32),
                            pltpu.VMEM((SLOTS, d_state, d_inner), jnp.float32),
                            pltpu.VMEM((SLOTS, 48, LANES), jnp.bfloat16),
                            pltpu.VMEM((SLOTS, 48, LANES), jnp.bfloat16),
                            pltpu.VMEM((2, 48, LANES), jnp.float32),
                            pltpu.VMEM((seg, d_inner), jnp.float32),
                            pltpu.VMEM((2, seg_count, per_device, d_state), jnp.float32),
                            pltpu.VMEM((3, layers, conv_dim), jnp.float32),
                            pltpu.VMEM((batch, 3, layers, conv_dim), jnp.bfloat16),
                            pltpu.SemaphoreType.DMA((layers,)),
                            pltpu.SemaphoreType.DMA((2,)),
                            pltpu.SemaphoreType.DMA((SLOTS, quads)),
                            pltpu.SemaphoreType.DMA((SLOTS, quads)),
                            pltpu.SemaphoreType.DMA((SLOTS, 2)),
                            pltpu.SemaphoreType.DMA((SLOTS, 2)),
                            pltpu.SemaphoreType.DMA((2, seg_count)),
                            pltpu.SemaphoreType.DMA,
                            pltpu.SemaphoreType.DMA((batch, seg_count)),
                            pltpu.SemaphoreType.DMA,
                            pltpu.SemaphoreType.REGULAR],
            compiler_params=pltpu.CompilerParams(dimension_semantics=('arbitrary',) * 2, vmem_limit_bytes=67043328, collective_id=0, has_side_effects=True),
        )(resid, jnp.swapaxes(w_in, 1, 2), w_out, *params)
        return out, state.reshape(batch, layers, heads // seg_count, head_dim, d_state), jnp.transpose(tail, (0, 2, 3, 1))

    return jax.shard_map(forward, mesh=mesh, in_specs=(P('dp', 'sp', None), P(), P(), P(), P(), P(), P(), P(), P(), P()), out_specs=(P('dp', 'sp', None), P('dp', None, 'sp', None, None), P('dp', None, None, None)), check_vma=False)
```

```python
import functools

import jax
import jax.numpy as jnp
from jax import lax
from jax.experimental import pallas as pl
from jax.experimental.pallas import tpu as pltpu
from jax.sharding import PartitionSpec as P

EPSILON = 1e-5
HALO = 8
SLOTS = 4
LANES = 128
LOG2_E = 1.4426950408889634


def softplus(v):
    return jnp.maximum(v, 0.0) + jnp.log1p(jnp.exp(-jnp.abs(v)))


def round_bf16(v):
    return v.astype(jnp.bfloat16).astype(jnp.float32)


def dot(a, b):
    return jnp.dot(a, b, preferred_element_type=jnp.float32)


def dot_nt(a, b):
    return lax.dot_general(a, b, (((1,), (1,)), ((), ())), preferred_element_type=jnp.float32)


def forward_kernel(dims, x_ref, w_in_hbm, w_out_hbm, pre_ref, conv_w_ref, conv_b_ref, dt_bias_ref, a_log_ref, d_skip_ref, gate_ref,
                   out_ref, state_hbm, tail_hbm,
                   res_ref, w_in_ref, w_out_ref, row_ref, expand_ref, u_ref, s_in_ref, s_out_ref, halo_in_ref, halo_out_ref, halo_f_ref, g_ref,
                   stage_ref, tail_f_ref, tail_ref,
                   w_sem, raw_sem, s_send, s_recv, halo_send, halo_recv, stage_send, stage_recv, tail_send, tail_recv, credit):
    d_inner, heads, seg, devices, batch = dims
    head_dim = d_inner // heads
    conv_dim = conv_b_ref.shape[1]
    tiles = conv_dim // LANES
    prompt = pl.program_id(0)
    layer = pl.program_id(1)
    me = lax.axis_index('sp')
    quad = 256
    sub = LANES
    quads = d_inner // quad
    bc = quads
    groups = ((bc, 0), tuple(range(1, quads)))
    spans = ((0, 16), (16, 32))
    spot = {b: (n, spans[n][0] + 6 * i) for n, group in enumerate(groups) for i, b in enumerate(group)}
    steps = batch * 2
    step = prompt * 2 + layer
    slots = s_in_ref.shape[0]
    slot = lax.rem(step, slots)
    last_device = devices - 1
    after = lax.rem(me + 1, devices)
    before = lax.rem(me + devices - 1, devices)
    tail_group = batch // tail_send.shape[0]
    per_device = d_inner // devices

    def w_in_copy(l):
        rows = pl.ds(0, w_in_hbm.shape[1])
        return pltpu.make_async_copy(w_in_hbm.at[l], w_in_ref.at[l, rows, :], raw_sem.at[l])

    def w_out_copy(l):
        return pltpu.make_async_copy(w_out_hbm.at[l], w_out_ref.at[l], w_sem.at[l])

    def remote(src, dst, send, recv, peer):
        return pltpu.make_async_remote_copy(src_ref=src, dst_ref=dst, send_sem=send, recv_sem=recv, device_id={'sp': peer},
                                            device_id_type=pl.DeviceIdType.MESH)

    def state_copy(n, q, peer):
        cols = pl.ds(q * quad, quad)
        return remote(s_out_ref.at[n, :, cols], s_in_ref.at[n, :, cols], s_send.at[n, q], s_recv.at[n, q], peer)

    def halo_copy(n, group, peer):
        rows = pl.ds(*spans[group])
        return remote(halo_out_ref.at[n, rows], halo_in_ref.at[n, rows], halo_send.at[n, group], halo_recv.at[n, group], peer)

    def stage_copy(n, p, l, peer):
        return remote(stage_ref.at[n, peer], state_hbm.at[p, l], stage_send.at[n, peer], stage_recv, peer)

    def stage_local(n, p, l):
        return pltpu.make_async_copy(stage_ref.at[n, me], state_hbm.at[p, l], stage_send.at[n, me])

    def tail_copy(group, peer):
        rows = pl.ds(group * tail_group, tail_group)
        return remote(tail_ref.at[rows], tail_hbm.at[rows], tail_send.at[group, peer], tail_recv, peer)

    def tail_local(group):
        rows = pl.ds(group * tail_group, tail_group)
        return pltpu.make_async_copy(tail_ref.at[rows], tail_hbm.at[rows], tail_send.at[group, me])

    left = lax.broadcasted_iota(jnp.int32, (sub, LANES), 1) < head_dim

    @pl.when(step == 0)
    def _():
        w_in_copy(0).start()
        w_out_copy(0).start()
        barrier = pltpu.get_barrier_semaphore()
        for k in range(1, devices):
            pl.semaphore_signal(barrier, inc=1, device_id={'sp': lax.rem(me + k, devices)}, device_id_type=pl.DeviceIdType.MESH)

        tail_f_ref[...] = jnp.zeros(tail_f_ref.shape, jnp.float32)
        halo_f_ref[...] = jnp.zeros(halo_f_ref.shape, jnp.float32)
        row_ref[...] = jnp.zeros(row_ref.shape, jnp.float32)

        @pl.when(me == 0)
        def _():
            s_in_ref[...] = jnp.zeros(s_in_ref.shape, jnp.float32)
            halo_in_ref[...] = jnp.zeros(halo_in_ref.shape, jnp.bfloat16)

        for l in range(2):
            for tap in range(4):
                row_ref[l, tap:tap + 1, 0:conv_dim] = 0.5 * conv_w_ref[l, tap:tap + 1, :]
            row_ref[l, 4:5, 0:conv_dim] = 0.5 * conv_b_ref[l:l + 1, :]
            row_ref[l, 5:6, 0:heads] = dt_bias_ref[l:l + 1, :]
            row_ref[l, 6:7, 0:heads] = -jnp.exp(a_log_ref[l:l + 1, :]) * LOG2_E
            for k in range(d_inner // LANES):
                d_left = jnp.broadcast_to(d_skip_ref[l:l + 1, 2 * k:2 * k + 1], (1, LANES))
                d_right = jnp.broadcast_to(d_skip_ref[l:l + 1, 2 * k + 1:2 * k + 2], (1, LANES))
                row_ref[l, 7:8, k * LANES:(k + 1) * LANES] = jnp.where(left[0:1], d_left, d_right)
        lane_head = lax.shift_right_logical(lax.broadcasted_iota(jnp.int32, expand_ref.shape, 1), 6)
        expand_ref[...] = jnp.where(lax.broadcasted_iota(jnp.int32, expand_ref.shape, 0) == lane_head, 1.0, 0.0).astype(jnp.bfloat16)

        pl.semaphore_wait(barrier, devices - 1)

    @pl.when(prompt == 0)
    def _():
        w_in_copy(layer).wait()
        w_out_copy(layer).wait()

        @pl.when(layer == 0)
        def _():
            w_in_copy(1).start()
            w_out_copy(1).start()

        w_in_ref[layer, w_in_hbm.shape[1]:, :] = jnp.zeros((w_in_ref.shape[1] - w_in_hbm.shape[1], w_in_ref.shape[2]), jnp.bfloat16)

    @pl.when((me < last_device) & (step >= slots))
    def _():
        for n in range(len(groups)):
            halo_copy(slot, n, after).wait_send()
        for q in range(quads):
            state_copy(slot, q, after).wait_send()
        pl.semaphore_wait(credit, 1)

    @pl.when(layer == 0)
    def _():
        res_ref[...] = x_ref[0]

    resid = res_ref[...]
    mean_sq = jnp.mean(resid * resid, axis=-1, keepdims=True)
    h = (resid * lax.rsqrt(mean_sq + EPSILON) * pre_ref[pl.ds(layer, 1), :]).astype(jnp.bfloat16)

    def project(b):
        first_col = b * quad
        u = round_bf16(dot_nt(h, w_in_ref[layer, d_inner + first_col:d_inner + first_col + quad, :]))
        for k in range(quad // LANES):
            j = first_col // LANES + k
            lanes = slice(k * LANES, (k + 1) * LANES)
            u_ref[j, HALO:HALO + seg, :] = u[:, lanes]
            group, first = spot[b]
            for tap in range(3):
                row = first + 2 * tap + k
                halo_f_ref[0, row:row + 1, :] = u_ref[j, HALO + seg - 3 + tap:HALO + seg - 2 + tap, :]

    def project_group(group):
        for b in groups[group]:
            project(b)
        first, count = spans[group]
        halo_out_ref[slot, first:first + count, :] = halo_f_ref[0, first:first + count, :].astype(jnp.bfloat16)

    def take_halo(group):
        first, count = spans[group]
        halo_f_ref[1, first:first + count, :] = halo_in_ref[slot, first:first + count, :].astype(jnp.float32)

    def conv(b):
        outs = []
        for j in range(b * quad // LANES, (b + 1) * quad // LANES):
            cols = slice(j * LANES, (j + 1) * LANES)
            group, first = spot[b]
            for tap in range(3):
                row = first + 2 * tap + j % 2
                u_ref[j, HALO - 3 + tap:HALO - 2 + tap, :] = halo_f_ref[1, row:row + 1, :]
            acc = row_ref[layer, 4:5, cols]
            for tap in range(4):
                acc = acc + u_ref[j, HALO - 3 + tap:HALO - 3 + tap + seg, :] * row_ref[layer, tap:tap + 1, cols]
            outs.append((acc + acc * jnp.tanh(acc)).astype(jnp.bfloat16))
        return outs

    dt_raw = round_bf16(dot_nt(h, w_in_ref[layer, d_inner + conv_dim:d_inner + conv_dim + LANES, :]))
    delta = softplus(dt_raw + row_ref[layer, 5:6, 0:LANES]).astype(jnp.bfloat16)
    project_group(0)

    @pl.when(me < last_device)
    def _():
        halo_copy(slot, 0, after).start()

    @pl.when(me > 0)
    def _():
        halo_copy(slot, 0, before).wait_recv()

    take_halo(0)
    b_act, c_act = conv(bc)
    causal = lax.broadcasted_iota(jnp.int32, (sub, sub), 0) >= lax.broadcasted_iota(jnp.int32, (sub, sub), 1)
    tri = jnp.where(causal, 1.0, 0.0).astype(jnp.bfloat16)
    b_t = jnp.transpose(b_act.astype(jnp.float32)).astype(jnp.bfloat16)
    subs = [slice(i * sub, (i + 1) * sub) for i in range(seg // sub)]
    cums = [dot(tri, delta[rows]) * row_ref[layer, 6:7, 0:LANES] for rows in subs]
    cums_t = [jnp.transpose(cum) for cum in cums]
    scores = [jnp.where(causal, dot_nt(c_act[rows], b_act[rows]), 0.0) for rows in subs]

    def local_part(q):
        cols = slice(q * quad, (q + 1) * quad)
        x_tiles = conv(q)
        if q + 1 < len(groups):
            project_group(q + 1)
        z = dot_nt(h, w_in_ref[layer, cols, :]).astype(jnp.bfloat16)
        dt_wide = dot(delta, expand_ref[:, cols])
        parts = []
        for i, rows in enumerate(subs):
            x_ends = []
            decays = []
            ys = []
            scales = []
            for k in range(quad // LANES):
                lanes = slice(k * LANES, (k + 1) * LANES)
                head = (q * quad + k * LANES) // head_dim
                x_float = x_tiles[k][rows].astype(jnp.float32)
                x_scaled = x_float * dt_wide[rows, lanes]
                x_dot = x_scaled.astype(jnp.bfloat16)
                wide = [jnp.broadcast_to(cums[i][:, head + n:head + n + 1], (sub, LANES)) for n in range(2)]
                mix = [(jnp.exp2(jnp.minimum(wide[n] - cums_t[i][head + n:head + n + 1, :], 0.0)) * scores[i]).astype(jnp.bfloat16) for n in range(2)]
                none = jnp.zeros_like(x_dot)
                pair_rhs = jnp.concatenate([jnp.where(left, x_dot, none), jnp.where(left, none, x_dot)], axis=0)
                y_intra = dot(jnp.concatenate(mix, axis=1), pair_rhs)
                cum_pair = jnp.where(left, wide[0], wide[1])
                last = cum_pair[sub - 1:sub, :]
                x_ends.append((x_scaled * jnp.exp2(last - cum_pair)).astype(jnp.bfloat16))
                decays.append(jnp.exp2(last))
                tile = slice(q * quad + k * LANES, q * quad + (k + 1) * LANES)
                ys.append(y_intra + row_ref[layer, 7:8, tile] * x_float)
                scales.append(jnp.exp2(cum_pair))
            added = dot(b_t[:, rows], jnp.concatenate(x_ends, axis=1))
            parts.append((jnp.concatenate(decays, axis=1), added, ys, scales))
        return z, parts

    def gate_part(q, z, parts, states, sums):
        for i, rows in enumerate(subs):
            y_inter = dot(c_act[rows], states[i].astype(jnp.bfloat16))
            for k in range(quad // LANES):
                lanes = slice(k * LANES, (k + 1) * LANES)
                y = parts[i][2][k] + y_inter[:, lanes] * parts[i][3][k]
                z_half = 0.5 * z[rows, lanes].astype(jnp.float32)
                gated = round_bf16(y) * (z_half + z_half * jnp.tanh(z_half))
                g_ref[rows, q * quad + k * LANES:q * quad + (k + 1) * LANES] = gated
                sums[i] = sums[i] + gated * gated

    sum_sq = [jnp.zeros((sub, LANES), jnp.float32) for _ in subs]
    z, parts = local_part(0)
    for q in range(quads):
        cols = slice(q * quad, (q + 1) * quad)

        @pl.when(me < last_device)
        def _():
            if q + 1 < len(groups):
                halo_copy(slot, q + 1, after).start()

        @pl.when(me > 0)
        def _():
            state_copy(slot, q, before).wait_recv()

        states = [s_in_ref[slot, :, cols]]
        for decay, added, _, _ in parts:
            states.append(states[-1] * decay + added)
        s_out_ref[slot, :, cols] = states[-1]

        @pl.when(me < last_device)
        def _():
            state_copy(slot, q, after).start()

        if q == 0:
            @pl.when(me > 0)
            def _():
                halo_copy(slot, 1, before).wait_recv()

            take_halo(1)
        gate_part(q, z, parts, states, sum_sq)
        if q + 1 < quads:
            z, parts = local_part(q + 1)

    @pl.when((me > 0) & (step < steps - slots))
    def _():
        pl.semaphore_signal(credit, inc=1, device_id={'sp': before}, device_id_type=pl.DeviceIdType.MESH)

    @pl.when(me == last_device)
    def _():
        n = lax.rem(step, 2)

        @pl.when(step >= 2)
        def _():
            stage_local(n, prompt - 1, layer).wait()
            for k in range(1, devices):
                stage_copy(n, prompt - 1, layer, lax.rem(me + k, devices)).wait_send()

        final = jnp.transpose(s_out_ref[slot])
        for k in range(devices):
            stage_ref[n, k] = final[k * per_device:(k + 1) * per_device, :]
        stage_local(n, prompt, layer).start()
        for k in range(1, devices):
            stage_copy(n, prompt, layer, lax.rem(me + k, devices)).start()

        for l in range(2):
            @pl.when(layer == l)
            def _():
                for j in range(tiles):
                    for k in range(3):
                        tail_f_ref[k, l:l + 1, j * LANES:(j + 1) * LANES] = u_ref[j, seg + HALO - 3 + k:seg + HALO - 2 + k, :]

        @pl.when(layer == 1)
        def _():
            tail_ref[prompt] = tail_f_ref[...].astype(jnp.bfloat16)

        @pl.when((layer == 1) & (lax.rem(prompt, tail_group) == tail_group - 1))
        def _():
            group = lax.div(prompt, tail_group)
            tail_local(group).start()
            for k in range(1, devices):
                tail_copy(group, lax.rem(me + k, devices)).start()

    for i, rows in enumerate(subs):
        scale = lax.rsqrt(jnp.sum(sum_sq[i], axis=-1, keepdims=True) * (1.0 / d_inner) + EPSILON)
        normed = (g_ref[rows, :] * scale * gate_ref[layer]).astype(jnp.bfloat16)
        res_ref[rows, :] = resid[rows] + dot(normed, w_out_ref[layer])

    @pl.when(layer == 1)
    def _():
        out_ref[0] = res_ref[...]

    @pl.when(step == steps - 1)
    def _():
        @pl.when(me < last_device)
        def _():
            for n in range(slots):
                for group in range(len(groups)):
                    halo_copy(n, group, after).wait_send()
                for q in range(quads):
                    state_copy(n, q, after).wait_send()
            pltpu.make_async_copy(state_hbm, state_hbm, stage_recv).wait()
            pltpu.make_async_copy(tail_hbm, tail_hbm, tail_recv).wait()

        @pl.when(me == last_device)
        def _():
            for n in range(2):
                stage_local(n, batch - 1, n).wait()
                for k in range(1, devices):
                    stage_copy(n, batch - 1, n, lax.rem(me + k, devices)).wait_send()
            @pl.loop(0, tail_send.shape[0])
            def _(group):
                tail_local(group).wait()
                for k in range(1, devices):
                    tail_copy(group, lax.rem(me + k, devices)).wait_send()


def solution(mesh):
    seg_count = mesh.shape['sp']

    def forward(resid, pre_norm, w_in, conv_w, conv_b, dt_bias, a_log, d_skip, gate_norm, w_out):
        batch, seg, d_model = resid.shape
        layers, d_inner, _ = w_out.shape
        heads = dt_bias.shape[1]
        head_dim = d_inner // heads
        conv_dim = conv_b.shape[1]
        d_state = (conv_dim - d_inner) // 2
        tiles = conv_dim // LANES
        per_device = d_inner // seg_count
        quads = d_inner // 256
        params = (pre_norm, jnp.swapaxes(conv_w, 1, 2), conv_b, dt_bias, a_log, d_skip, gate_norm)

        def whole(a):
            return pl.BlockSpec(a.shape, lambda p, l: (0,) * a.ndim, pipeline_mode=pl.Buffered(1))

        hbm = pl.BlockSpec(memory_space=pl.ANY)
        block = pl.BlockSpec((1, seg, d_model), lambda p, l: (p, 0, 0))
        out, state, tail = pl.pallas_call(
            functools.partial(forward_kernel, (d_inner, heads, seg, seg_count, batch)),
            grid=(batch, layers),
            out_shape=(jax.ShapeDtypeStruct((batch, seg, d_model), jnp.float32),
                       jax.ShapeDtypeStruct((batch, layers, per_device, d_state), jnp.float32),
                       jax.ShapeDtypeStruct((batch, 3, layers, conv_dim), jnp.bfloat16)),
            in_specs=[block, hbm, hbm] + [whole(a) for a in params],
            out_specs=(block, hbm, hbm),
            scratch_shapes=[pltpu.VMEM((seg, d_model), jnp.float32),
                            pltpu.VMEM((layers, d_inner + conv_dim + LANES, d_model), jnp.bfloat16),
                            pltpu.VMEM(w_out.shape, jnp.bfloat16),
                            pltpu.VMEM((layers, 8, conv_dim), jnp.float32),
                            pltpu.VMEM((LANES, d_inner), jnp.bfloat16),
                            pltpu.VMEM((tiles, HALO + seg, LANES), jnp.float32),
                            pltpu.VMEM((SLOTS, d_state, d_inner), jnp.float32),
                            pltpu.VMEM((SLOTS, d_state, d_inner), jnp.float32),
                            pltpu.VMEM((SLOTS, 48, LANES), jnp.bfloat16),
                            pltpu.VMEM((SLOTS, 48, LANES), jnp.bfloat16),
                            pltpu.VMEM((2, 48, LANES), jnp.float32),
                            pltpu.VMEM((seg, d_inner), jnp.float32),
                            pltpu.VMEM((2, seg_count, per_device, d_state), jnp.float32),
                            pltpu.VMEM((3, layers, conv_dim), jnp.float32),
                            pltpu.VMEM((batch, 3, layers, conv_dim), jnp.bfloat16),
                            pltpu.SemaphoreType.DMA((layers,)),
                            pltpu.SemaphoreType.DMA((2,)),
                            pltpu.SemaphoreType.DMA((SLOTS, quads)),
                            pltpu.SemaphoreType.DMA((SLOTS, quads)),
                            pltpu.SemaphoreType.DMA((SLOTS, 2)),
                            pltpu.SemaphoreType.DMA((SLOTS, 2)),
                            pltpu.SemaphoreType.DMA((2, seg_count)),
                            pltpu.SemaphoreType.DMA,
                            pltpu.SemaphoreType.DMA((batch, seg_count)),
                            pltpu.SemaphoreType.DMA,
                            pltpu.SemaphoreType.REGULAR],
            compiler_params=pltpu.CompilerParams(dimension_semantics=('arbitrary',) * 2, vmem_limit_bytes=67043328, collective_id=0, has_side_effects=True),
        )(resid, jnp.swapaxes(w_in, 1, 2), w_out, *params)
        return out, state.reshape(batch, layers, heads // seg_count, head_dim, d_state), jnp.transpose(tail, (0, 2, 3, 1))

    return jax.shard_map(forward, mesh=mesh, in_specs=(P('dp', 'sp', None), P(), P(), P(), P(), P(), P(), P(), P(), P()), out_specs=(P('dp', 'sp', None), P('dp', None, 'sp', None, None), P('dp', None, None, None)), check_vma=False)
```
